32 devices in a mesh: pix: 32 (over z, y, x, core).
Axes of the slice: x: 2, y: 2, z: 4, core: 2. Of those that a mesh axis runs over, the one named last changes fastest.
Arguments:
- green: float32 [2048, 6144], P('pix'), may hold values from -200 to 200, as said below
- sketch: float32 [6144, 128], P('pix'), may hold values from -0.078125 to 0.078125
Outputs:
- basis: float32 [2048, 128], P('pix')
- projection: float32 [6144, 128], P('pix')
- spectrum_gram: float32 [128, 128], replicated
The draws below stay inside these ranges and needn't reach their ends.
Inputs may be any that keep to these rules, and one draw needn't show every extreme that they name: `green`: finite real entries; each patch's column has its own scale.
All inputs are finite; a program needn't handle non-finite values.
Results may differ from the reference program's by a relative error of at most 0.000086.
Values sent between devices are 32-bit elements; how exact they have to be, the bound alone decides.
A program may use at most 64 MiB of HBM per device.

```python
import jax
import jax.numpy as jnp
from jax import lax

PATCHES = 6144
RANK = 128
PIXELS = 2048


def draw_green(key, part):
    key_cols = jax.random.fold_in(key, 11)
    key_vals = jax.random.fold_in(key, 12)
    col_scale = jnp.exp(jax.random.uniform(key_cols, (1, PATCHES), jnp.float32, jnp.log(0.3), jnp.log(3.0)))
    values = jnp.clip(jax.random.normal(key_vals, (PIXELS, PATCHES), jnp.float32), -6.0, 6.0)
    return values * col_scale


def block_scale(stream_key, shape, pieces, least, largest):
    factor_of, own = 1.0, jax.random.fold_in(stream_key, 6)
    for dim, shards_of in pieces:
        steps = jnp.exp(jax.random.uniform(jax.random.fold_in(own, dim), (shards_of,), jnp.float32, least / len(pieces), largest / len(pieces)))
        factor_of = factor_of * jnp.repeat(steps, shape[dim] // shards_of).reshape([-1 if axis == dim else 1 for axis in range(len(shape))])
    return factor_of


def noise(stream_key, shape, spread, limit, shards=(), kind=jnp.bfloat16):
    values = spread * jax.random.normal(stream_key, shape, jnp.float32)
    if shards:
        values = values * block_scale(stream_key, shape, shards, -0.22, 0.18)
    return jnp.clip(values, -limit, limit).astype(kind)


def setup_inputs(seed: int = 0) -> dict:
    arg_keys = jax.random.split(jax.random.key(seed), 3)
    return {
        "green": draw_green(jax.random.fold_in(arg_keys[2], 71), 0),
        "sketch": noise(arg_keys[1], (PATCHES, RANK), PATCHES ** -0.5, 0.078125, ((0, 32),), jnp.float32),
    }


def reference(green, sketch):
    highest = lax.Precision.HIGHEST
    sketched = jnp.dot(green.astype(jnp.float32), sketch.astype(jnp.float32), precision=highest, preferred_element_type=jnp.float32)
    gram = jnp.dot(sketched.T.astype(jnp.float32), sketched.astype(jnp.float32), precision=highest, preferred_element_type=jnp.float32)
    lower = jnp.linalg.cholesky(gram)
    orthonormal = jax.scipy.linalg.solve_triangular(lower, sketched.T, lower=True).T
    basis = jnp.sqrt(jnp.float32(PIXELS)) * orthonormal
    projection = jnp.dot(green.T.astype(jnp.float32), orthonormal.astype(jnp.float32), precision=highest, preferred_element_type=jnp.float32)
    spectrum_gram = jnp.dot(projection.T.astype(jnp.float32), projection.astype(jnp.float32), precision=highest, preferred_element_type=jnp.float32) / jnp.float32(PATCHES)
    return (basis, projection, spectrum_gram)
```

```python
import functools
import math

import jax
import jax.numpy as jnp
from jax import lax
from jax.experimental import pallas as pl
from jax.experimental.pallas import tpu as pltpu
from jax.sharding import PartitionSpec as P

MESH = pl.DeviceIdType.MESH
F32 = jnp.float32
BF16 = jnp.bfloat16
PANEL = 8
PARTS = 8


def grid_of(devices):
    cores = 2 if devices % 2 == 0 else 1
    chips = devices // cores
    side = 1
    for k in range(1, chips + 1):
        if chips % (k * k) == 0 and k * k * k <= chips:
            side = k
    return cores, side, side, chips // (side * side)


def order_of(planes):
    table = []
    for z in range(planes):
        rest = sorted((k for k in range(planes) if k != z), key=lambda k: (abs(k - z), k))
        if planes % 2 == 0:
            rest.remove(z ^ 1)
            rest.insert(0, z ^ 1)
        table.append([z] + rest)
    return table


def layout_of(rows, rank):
    parts = 2 if rows % 32 == 0 and rank == 128 else 1
    deep = rows // parts
    return parts, deep, (deep // 2 + 7) // 8 * 8


PLANS = {
    (2, 4): [
        ("ownz", 0, 1), ("ownp", 1), ("ownp", 0), ("ownz", 0, 2), ("ownz", 0, 3), ("zin", 0, 1),
        ("diag", 0, 0), ("ownz", 1, 1), ("zin", 0, 2), ("prep", 1), ("ownz", 1, 2), ("prep", 3),
        ("zin", 0, 3), ("diag", 0, 1), ("ownz", 1, 3), ("prep", 0), ("zin", 1, 1), ("diag", 0, 2),
        ("diag", 0, 3), ("zin", 1, 2), ("zin", 1, 3), ("diag", 1, 1), ("diag", 1, 0), ("fin", 0, 1),
        ("prep", 2), ("fin", 0, 2), ("fin", 0, 3), ("fin", 0, 0), ("diag", 1, 2), ("give", 0),
        ("diag", 1, 3), ("take", 0), ("rs1", 0, 0), ("rs1", 0, 2), ("fin", 1, 1), ("fin", 1, 2),
        ("rs1", 0, 1), ("rs1", 0, 3), ("fin", 1, 0), ("fin", 1, 3), ("give", 1), ("rs2", 0, 2),
        ("take", 1), ("sum", 0, 0), ("rs1", 1, 3), ("rs2", 0, 3), ("rs2", 0, 1), ("rs1", 1, 2),
        ("rs3", 0, 2), ("rs2", 1, 3), ("sum", 0, 1), ("rs1", 1, 1), ("rs3", 0, 3), ("rs1", 1, 0),
        ("rs2", 1, 2), ("rs3", 1, 3), ("rs2", 1, 1), ("rs2", 0, 0), ("sum", 0, 2), ("rs2", 1, 0),
        ("rs3", 0, 1), ("rs3", 1, 2), ("rs3", 1, 1), ("sum", 0, 3), ("panel", 0), ("rs3", 0, 0),
        ("rs3", 1, 0), ("collect",), ("sum", 1, 0), ("panel", 1), ("panel", 2), ("panel", 3),
        ("sum", 1, 1), ("panel", 4), ("panel", 5), ("sum", 1, 2), ("panel", 6), ("panel", 7), ("finish",),
        ("sum", 1, 3),
    ],
}


def schedule(parts, planes):
    tuned = PLANS.get((parts, planes))
    if tuned:
        return tuned
    near = range(planes)
    far = near[::-1]
    plan = []
    for h in range(parts):
        plan += [("ownp", h)] + [("ownz", h, p) for p in near[1:]]
    for h in range(parts):
        for p in near:
            plan += [("zin", h, p)] * (p > 0) + [("diag", h, p)]
    plan += [("prep", p) for p in near]
    for h in range(parts):
        plan += [("fin", h, p) for p in near] + [("give", h)]
    plan += [("take", h) for h in range(parts)] + [("sum", 0, 0)]
    for h in range(parts):
        for p in far:
            plan += [("rs1", h, p), ("rs2", h, p), ("rs3", h, p)]
    plan += [("sum", 0, 1), ("sum", 0, 2), ("collect",), ("sum", 1, 0), ("sum", 0, 3)]
    plan += [("sum", 1, 1)] + [("panel", i) for i in range(PARTS)] + [("finish",)]
    return plan + [("sum", 1, 2), ("sum", 1, 3)]

def split(v):
    hi = v.astype(BF16)
    return hi, (v - hi.astype(F32)).astype(BF16)


def thirds(v):
    a = v.astype(BF16).astype(F32)
    b = (v - a).astype(BF16).astype(F32)
    return a, b, v - a - b


def dot(a, b, dims=((1,), (0,))):
    return lax.dot_general(a, b, (dims, ((), ())), preferred_element_type=F32)


def exact(a, b, dims=((1,), (0,))):
    return lax.dot_general(
        a, b, (dims, ((), ())), precision=lax.Precision.HIGHEST, preferred_element_type=F32
    )


def kernel(grid, total_pixels, green_in, sketch_in, basis, projection, inverse_out, spec, scratch):
    C, X, Y, Z = grid
    assert C == 2
    r = scratch
    me = lax.axis_index("pix")
    c = lax.rem(me, C)
    x = lax.rem(me // C, X)
    y = lax.rem(me // (C * X), Y)
    z = me // (C * X * Y)
    green, sketch, gat, part = r["green"], r["sketch"], r["gat"], r["part"]
    rows, rank = sketch.shape
    pixels = green_in.shape[0]
    both = C * pixels
    G, deep, half = layout_of(rows, rank)
    wide = rank // G
    slab = X * Y * C * rows
    table = order_of(Z)
    mine = pl.ds(pl.multiple_of(c * pixels, 8), pixels)
    low, high = pl.ds(0, half), pl.ds(half, deep - half)
    spans = (low, high)

    def dev(zz, yy, xx, cc):
        return (((zz * Y + yy) * X + xx) * C + cc,)

    def at(v, d, n):
        return lax.rem(v + d + n, n)

    def near(p):
        out = table[0][p]
        for k in range(1, Z):
            out = jnp.where(z == k, table[k][p], out)
        return out

    partner = dev(z, y, x, 1 - c)
    dxs, dys = range(1, X), range(1, Y)
    counter = [0]
    sends = []

    sent = [0]

    def copy(src, dst, recv, to):
        pltpu.make_async_remote_copy(
            src_ref=src, dst_ref=dst, send_sem=r["send"].at[0], recv_sem=recv,
            device_id=to, device_id_type=MESH,
        ).start()
        sent[0] += math.prod(src.shape) // rank

    def tally(count):
        ref = r["tally"].at[pl.ds(0, count)]
        return pltpu.make_async_remote_copy(
            src_ref=ref, dst_ref=ref, send_sem=r["send"].at[0], recv_sem=r["send"].at[0],
            device_id=partner, device_id_type=MESH,
        )

    def arrive(recv, count):
        ref = r["tally"].at[pl.ds(0, count)]
        pltpu.make_async_remote_copy(
            src_ref=ref, dst_ref=ref, send_sem=r["send"].at[0], recv_sem=recv,
            device_id=partner, device_id_type=MESH,
        ).wait_recv()

    def finish_sends():
        tally(sent[0]).wait_send()

    load_sketch = pltpu.make_async_copy(sketch_in, sketch, r["load"].at[0])
    load_green = pltpu.make_async_copy(green_in, green.at[mine], r["load"].at[1])
    load_sketch.start()
    load_green.start()
    barrier = pltpu.get_barrier_semaphore()
    peers = [(partner, None)]
    peers += [(dev(z, y, at(x, dx, X), c), None) for dx in dxs]
    peers += [(dev(z, at(y, dy, Y), x, c), None) for dy in dys]
    peers += [(dev(z - 1, y, x, c), z > 0), (dev(z + 1, y, x, c), z < Z - 1)]

    def greet(peer):
        pl.semaphore_signal(barrier, inc=1, device_id=peer, device_id_type=MESH)

    for peer, when in peers:
        if when is None:
            greet(peer)
        else:
            pl.when(when)(functools.partial(greet, peer))
    lanes = lax.broadcasted_iota(jnp.int32, (deep, rank), 1)
    load_sketch.wait()
    if G == 1:
        gat[0, z, y, x] = sketch[...]
    else:
        top, bottom = sketch[:deep], sketch[deep:]
        gat[0, z, y, x] = jnp.where(lanes < wide, top, pltpu.roll(bottom, wide, 1))
        gat[1, z, y, x] = jnp.where(lanes < wide, pltpu.roll(top, wide, 1), bottom)
    known = len(peers) - 2 + jnp.where(z > 0, 1, 0) + jnp.where(z < Z - 1, 1, 0)
    pl.semaphore_wait(barrier, known)

    rest = deep - half

    def along_x(h, s, k):
        ref = gat.at[h, near(s), y, x, spans[k]]
        for dx in dxs:
            copy(ref, ref, r["agr" if k else "agf"].at[h, s], dev(z, y, at(x, dx, X), c))

    def along_y(h, s, k):
        ref = gat.at[h, near(s), y, x, spans[k]]
        for dy in dys:
            copy(ref, ref, r["agf" if k else "agr"].at[h, s], dev(z, at(y, dy, Y), x, c))

    def in_plane(h, s):
        along_x(h, s, 0)
        along_y(h, s, 1)
        along_x(h, s, 1)
        along_y(h, s, 0)

    def tell(sem, to):
        pl.semaphore_signal(sem, inc=1, device_id=to, device_id_type=MESH)

    def learn(j):
        up, down = r["kup"].at[j], r["kdown"].at[j]
        pl.when((z >= 1) & (z + j < Z))(functools.partial(tell, up, dev(z - 1, y, x, c)))
        pl.when((z + 1 < Z) & (z - j >= 0))(functools.partial(tell, down, dev(z + 1, y, x, c)))

    def known_far(j):
        pl.when(z + 1 + j < Z)(lambda: pl.semaphore_wait(r["kup"].at[j], 1))
        pl.when(z - 1 - j >= 0)(lambda: pl.semaphore_wait(r["kdown"].at[j], 1))

    reach = [0]

    def to_plane(h, p):
        far = max(abs(row[p] - row[0]) for row in table)
        while reach[0] < far - 1:
            reach[0] += 1
            learn(reach[0])
            known_far(reach[0])
        ref = gat.at[h, z, y, x]
        copy(ref, ref, r["agz"].at[h, z], dev(near(p), y, x, c))

    def zin(h, s):
        arrive(r["agz"].at[h, near(s)], deep)
        in_plane(h, s)

    def diag(h, s):
        zc = near(s)
        if dxs or dys:
            arrive(r["agf"].at[h, s], len(dxs) * half + len(dys) * rest)
        for dx in dxs:
            for dy in dys:
                ref = gat.at[h, zc, y, at(x, -dx, X), low]
                copy(ref, ref, r["agr"].at[h, s], dev(z, at(y, dy, Y), x, c))
        for dy in dys:
            for dx in dxs:
                ref = gat.at[h, zc, at(y, -dy, Y), x, high]
                copy(ref, ref, r["agr"].at[h, s], dev(z, y, at(x, dx, X), c))

    def swap():
        pltpu.make_async_remote_copy(
            src_ref=green_in, dst_ref=green.at[mine], send_sem=r["swap_send"].at[0], recv_sem=r["swap"].at[0],
            device_id=partner, device_id_type=MESH,
        ).start()

    def swapped():
        other = green.at[pl.ds(pl.multiple_of((1 - c) * pixels, 8), pixels)]
        load_green.wait()
        pltpu.make_async_remote_copy(
            src_ref=green_in, dst_ref=other, send_sem=r["swap_send"].at[0], recv_sem=r["swap"].at[0],
            device_id=partner, device_id_type=MESH,
        ).wait()

    gl, gt, turned = r["gl"], r["gt"], r["turned"]

    def prep(s):
        g = green[:, pl.ds(pl.multiple_of(near(s) * slab, 128), slab)]
        turned[...] = g.T
        for w in range(X * Y):
            block = turned[pl.ds(pl.multiple_of(w * C * rows + c * rows, 8), rows)]
            hi, lo = split(block)
            gt[s, w] = jnp.concatenate(
                [v[g * deep : (g + 1) * deep] for g in range(G) for v in (hi, lo)], axis=1
            )
            halves = [split(block[g * deep : (g + 1) * deep].T) for g in range(G)]
            gl[s, w] = jnp.concatenate([v[0] for v in halves] + [v[1] for v in halves], axis=0)

    started = set()

    def multiply(h, s):
        if dxs or dys:
            arrive(r["agr"].at[h, s], len(dxs) * rest + len(dys) * half + len(dxs) * len(dys) * deep)
        zc = near(s)
        out = None
        for w in range(X * Y):
            b_hi, b_lo = split(gat[h, zc, w // X, w % X])
            tall = dot(gl[s, w], b_hi)
            term = tall[: G * both] + tall[G * both :] + dot(gl[s, w, : G * both], b_lo)
            out = term if out is None else out + term
        if h in started:
            r["acc"][h] += out
        else:
            started.add(h)
            r["acc"][h] = out

    lane_b = lax.broadcasted_iota(jnp.int32, (both, rank), 1)

    def give(h):
        v = r["acc"][h]
        if G == 2:
            v = jnp.where(lane_b < wide, v[:both], v[both:])
        r["mine"][h] = v
        copy(r["mine"].at[h], r["theirs"].at[h], r["swap"].at[1 + h], partner)

    weights = {}

    def take(h):
        arrive(r["swap"].at[1 + h], both)
        v = r["mine"][h] + r["theirs"][h]
        if G == 2:
            v = v + pltpu.roll(v, wide, 1)
        r["folded"][h] = v
        tall = [v] if G == 1 else [jnp.where(lane_b < wide, v, 0.0), jnp.where(lane_b < wide, 0.0, v)]
        pairs = [split(t) for t in tall]
        for i in range(2):
            r["weights"][h, i] = jnp.concatenate([p[i] for p in pairs for _ in range(2)], axis=0)

    def merge():
        if G == 1:
            r["sketched"][...] = r["folded"][0]
        else:
            r["sketched"][...] = jnp.where(lane_b < wide, r["folded"][0], r["folded"][1])

    here = y * X + x
    q = rank // (C * X * Y)
    cores = [(dy, dx, dc) for dy in range(Y) for dx in range(X) for dc in range(C) if (dy, dx, dc) != (0, 0, 0)]

    def total_sum(k, value, per_chip):
        src, inc, top, res = (r[n].at[k] for n in ("t_src", "t_in", "t_top", "t_res"))
        first = [v for v in cores if not (per_chip and v[2])]

        def step0():
            v = value()
            for i in range(C):
                for w in range(X * Y):
                    begin = (i * X * Y + w) * q
                    src[i, w] = v[begin : begin + q]
            for n, (dy, dx, dc) in enumerate(first):
                yy, xx, cc = at(y, dy, Y), at(x, dx, X), lax.rem(c + dc, C)
                copy(src.at[cc, yy * X + xx], inc.at[n], r["sums"].at[k, 0], dev(z, yy, xx, cc))

        def step1():
            total = src[c, here]
            arrive(r["sums"].at[k, 0], len(first) * q)
            for n in range(len(first)):
                total = total + inc[n]
            top[z] = total
            for p in range(1, Z):
                copy(top.at[z], top.at[z], r["sums"].at[k, 1], dev(near(p), y, x, c))

        def step2():
            if Z > 1:
                arrive(r["sums"].at[k, 1], (Z - 1) * q)
            res[c, here] = jnp.sum(top[...], axis=0)
            for n, (dy, dx, dc) in enumerate(cores):
                yy, xx, cc = at(y, dy, Y), at(x, dx, X), lax.rem(c + dc, C)
                copy(res.at[c, here], res.at[c, here], r["sums"].at[k, 2], dev(z, yy, xx, cc))

        def step3():
            arrive(r["sums"].at[k, 2], len(cores) * q)

        def total():
            return jnp.concatenate([res[i, w] for i in range(C) for w in range(X * Y)], axis=0)

        return [step0, step1, step2, step3], total

    def rs1(h, s):
        for w in range(X * Y):
            part[h, s, w // X, w % X] = dot(gt[s, w], r["weights"][h, 0]) + dot(gt[s, w], r["weights"][h, 1])
        for dy in dys:
            for dx in dxs:
                yy, xx = at(y, dy, Y), at(x, dx, X)
                copy(part.at[h, s, yy, xx, low], r["rda"].at[h, s, dy, dx], r["rsf"].at[h, s],
                     dev(z, yy, x, c))
                copy(part.at[h, s, yy, xx, high], r["rdb"].at[h, s, dy, dx], r["rsf"].at[h, s],
                     dev(z, y, xx, c))
        for dy in dys:
            yy = at(y, dy, Y)
            copy(part.at[h, s, yy, x, low], r["rya"].at[h, s, dy], r["rsr"].at[h, s], dev(z, yy, x, c))
        for dx in dxs:
            xx = at(x, dx, X)
            copy(part.at[h, s, y, xx, high], r["rxb"].at[h, s, dx], r["rsr"].at[h, s], dev(z, y, xx, c))

    def rs2(h, s):
        if dxs and dys:
            arrive(r["rsf"].at[h, s], len(dxs) * len(dys) * deep)
        for dx in dxs:
            xx = at(x, dx, X)
            ref = part.at[h, s, y, xx, low]
            total = ref[...]
            for dy in dys:
                total = total + r["rda"][h, s, dy, dx]
            ref[...] = total
            copy(ref, r["rxa"].at[h, s, dx], r["rsr"].at[h, s], dev(z, y, xx, c))
        for dy in dys:
            yy = at(y, dy, Y)
            ref = part.at[h, s, yy, x, high]
            total = ref[...]
            for dx in dxs:
                total = total + r["rdb"][h, s, dy, dx]
            ref[...] = total
            copy(ref, r["ryb"].at[h, s, dy], r["rsr"].at[h, s], dev(z, yy, x, c))

    fin = r["fin"]

    def rs3(h, s):
        if dxs or dys:
            arrive(r["rsr"].at[h, s], (len(dxs) + len(dys)) * deep)
        total = part[h, s, y, x, low]
        for name, ds in (("rya", dys), ("rxa", dxs)):
            for d in ds:
                total = total + r[name][h, s, d]
        fin[h, s, low] = total
        total = part[h, s, y, x, high]
        for name, ds in (("rxb", dxs), ("ryb", dys)):
            for d in ds:
                total = total + r[name][h, s, d]
        fin[h, s, high] = total
        if s:
            copy(fin.at[h, s], r["rz"].at[h, z], r["rsz"].at[h], dev(near(s), y, x, c))

    def collect():
        got = []
        for h in range(G):
            total = fin[h, 0]
            if Z > 1:
                arrive(r["rsz"].at[h], (Z - 1) * deep)
            for p in range(1, Z):
                total = total + r["rz"][h, near(p)]
            got.append(total)
        if G == 1:
            r["raw"][...] = got[0]
        else:
            r["raw"][:deep] = jnp.where(lanes < wide, got[0], pltpu.roll(got[1], wide, 1))
            r["raw"][deep:] = jnp.where(lanes < wide, pltpu.roll(got[0], wide, 1), got[1])

    aug = r["aug"]
    lane = lax.broadcasted_iota(jnp.int32, (rank, rank), 1)
    row_of = lax.broadcasted_iota(jnp.int32, (rank, rank), 0)

    def eliminate(p, _):
        first = pl.multiple_of(p * PANEL, PANEL)
        lanes = lane[:PANEL]
        index = row_of[:PANEL, :1]
        block = aug[pl.ds(first, PANEL), :]
        left = block[:, :rank]
        cols = [
            jnp.sum(jnp.where(lanes == first + k, left, 0.0), axis=1, keepdims=True)
            for k in range(PANEL)
        ]
        scale = jnp.zeros((PANEL, 1), F32)
        for k in range(PANEL):
            inv = 1.0 / cols[k][k : k + 1]
            f = jnp.where(index > k, cols[k] * inv, 0.0)
            for m in range(k + 1, PANEL):
                cols[m] = cols[m] - f * cols[m][k : k + 1]
            block = block - f * block[k : k + 1]
            scale = jnp.where(index == k, inv, scale)
        u = thirds(jnp.where(lanes >= first + PANEL, block[:, :rank] * scale, 0.0))
        v = thirds(block)
        lhs = jnp.concatenate([u[i] for i in (0, 0, 0, 1, 1, 2)], axis=0).astype(BF16)
        rhs = jnp.concatenate([v[i] for i in (0, 1, 2, 0, 1, 0)], axis=0).astype(BF16)
        aug[...] = aug[...] - dot(lhs, rhs, ((0,), (0,)))
        aug[pl.ds(first, PANEL), :] = block
        return 0

    def begin():
        aug[:, :rank] = gram_total()
        aug[:, rank:] = jnp.where(lane == row_of, 1.0, 0.0)

    def chol(first, last):
        lax.fori_loop(first, last, eliminate, 0)

    def finish():
        diag = jnp.sum(jnp.where(lane == row_of, aug[:, :rank], 0.0), axis=1, keepdims=True)
        inverse = aug[:, rank:] * lax.rsqrt(diag)
        inverse_out[...] = inverse
        basis[...] = jnp.sqrt(F32(total_pixels)) * exact(r["sketched"][mine], inverse, ((1,), (1,)))
        projection[...] = exact(r["raw"][...], inverse, ((1,), (1,)))

    def gram_part():
        v = r["sketched"][...]
        return exact(v, v, ((0,), (0,)))

    def raw_part():
        v = r["raw"][...]
        return exact(v, v, ((0,), (0,)))

    gram, gram_total = total_sum(0, gram_part, True)
    spectrum, spectrum_total = total_sum(1, raw_part, False)
    panels = rank // PANEL

    def panel(i):
        if i == 0:
            begin()
        chol(panels * i // PARTS, panels * (i + 1) // PARTS)

    def send_own(h):
        in_plane(h, 0)
        if h == 0:
            swap()

    def give_take(h):
        take(h)
        if h == G - 1:
            merge()

    def prepare(s):
        if not prepared:
            swapped()
        prepared.add(s)
        prep(s)

    prepared = set()
    steps = dict(
        ownp=send_own, ownz=to_plane, prep=prepare, zin=zin, diag=diag, fin=multiply, give=give,
        take=give_take, rs1=rs1, rs2=rs2, rs3=rs3, collect=collect, sum=lambda k, i: (gram, spectrum)[k][i](),
        panel=panel, finish=finish,
    )
    for name, *index in schedule(G, Z):
        steps[name](*index)
    spec[...] = spectrum_total()
    finish_sends()


def finish_kernel(patches, basis_in, projection_in, inverse_in, spec_in, basis, projection, spectrum):
    inverse = inverse_in[...]
    basis[...] = basis_in[...]
    projection[...] = projection_in[...]
    spectrum[...] = exact(exact(inverse, spec_in[...]), inverse, ((1,), (1,))) / F32(patches)


def body(grid, green, sketch):
    C, X, Y, Z = grid
    rows, rank = sketch.shape
    pixels, patches = green.shape
    G, deep, half = layout_of(rows, rank)
    other = deep - half
    both = C * pixels
    plane = C * X * Y - 1
    few = rank // (C * X * Y)

    def vmem(*shape):
        return pltpu.VMEM(shape, F32)

    def packed(*shape):
        return pltpu.VMEM(shape, BF16)

    def dma(*shape):
        return pltpu.SemaphoreType.DMA(shape)

    flags = pltpu.SemaphoreType.REGULAR((Z,))
    links = X - 1 + Y - 1 + (X - 1) * (Y - 1)
    count = 2 * G * deep * (Z * links + Z - 1) + G * both + 2 * (2 * plane + Z) * few
    scratch = dict(
        green=vmem(both, patches), sketch=vmem(rows, rank), gat=vmem(G, Z, Y, X, deep, rank),
        turned=vmem(X * Y * C * rows, both),
        gl=packed(Z, X * Y, 2 * G * both, deep), gt=packed(Z, X * Y, deep, 2 * G * both),
        acc=vmem(G, G * both, rank), mine=vmem(G, both, rank), theirs=vmem(G, both, rank),
        folded=vmem(G, both, rank), weights=packed(G, 2, 2 * G * both, rank), sketched=vmem(both, rank),
        part=vmem(G, Z, Y, X, deep, rank),
        rda=vmem(G, Z, Y, X, half, rank), rdb=vmem(G, Z, Y, X, other, rank),
        rya=vmem(G, Z, Y, half, rank), rxb=vmem(G, Z, X, other, rank),
        rxa=vmem(G, Z, X, half, rank), ryb=vmem(G, Z, Y, other, rank),
        fin=vmem(G, Z, deep, rank), rz=vmem(G, Z, deep, rank), raw=vmem(rows, rank),
        t_src=vmem(2, C, X * Y, few, rank), t_in=vmem(2, plane, few, rank),
        t_top=vmem(2, Z, few, rank), t_res=vmem(2, C, X * Y, few, rank),
        aug=vmem(rank, 2 * rank), kup=flags, kdown=flags,
        tally=vmem(count, rank),
        send=dma(1), load=dma(2), swap=dma(1 + G), swap_send=dma(1),
        agz=dma(G, Z), agf=dma(G, Z), agr=dma(G, Z),
        rsf=dma(G, Z), rsr=dma(G, Z), rsz=dma(G), sums=dma(2, 3),
    )
    total_pixels = pixels * C * X * Y * Z
    tall = jax.ShapeDtypeStruct((pixels, rank), F32)
    wide = jax.ShapeDtypeStruct((rows, rank), F32)
    square = jax.ShapeDtypeStruct((rank, rank), F32)
    whole = pl.BlockSpec(memory_space=pltpu.VMEM)
    parts = pl.pallas_call(
        functools.partial(kernel, grid, total_pixels),
        out_shape=(tall, wide, square, square),
        in_specs=[pl.BlockSpec(memory_space=pl.ANY)] * 2,
        out_specs=(whole,) * 4,
        scratch_shapes=[scratch],
        compiler_params=pltpu.CompilerParams(
            collective_id=0, has_side_effects=True, vmem_limit_bytes=63 * 1024 * 1024
        ),
    )(green, sketch)
    return pl.pallas_call(
        functools.partial(finish_kernel, patches),
        out_shape=(tall, wide, square),
        in_specs=[whole] * 4,
        out_specs=(whole,) * 3,
    )(*parts)


def solution(mesh):
    grid = grid_of(mesh.shape["pix"])
    in_specs = (P("pix", None), P("pix", None))
    out_specs = (P("pix", None), P("pix", None), P())
    return jax.shard_map(
        functools.partial(body, grid), mesh=mesh, in_specs=in_specs, out_specs=out_specs, check_vma=False
    )
```

```python
import functools
import math

import jax
import jax.numpy as jnp
from jax import lax
from jax.experimental import pallas as pl
from jax.experimental.pallas import tpu as pltpu
from jax.sharding import PartitionSpec as P

MESH = pl.DeviceIdType.MESH
F32 = jnp.float32
BF16 = jnp.bfloat16
PANEL = 8
PARTS = 8


def grid_of(devices):
    cores = 2 if devices % 2 == 0 else 1
    chips = devices // cores
    side = 1
    for k in range(1, chips + 1):
        if chips % (k * k) == 0 and k * k * k <= chips:
            side = k
    return cores, side, side, chips // (side * side)


def order_of(planes):
    table = []
    for z in range(planes):
        rest = sorted((k for k in range(planes) if k != z), key=lambda k: (abs(k - z), k))
        if planes % 2 == 0:
            rest.remove(z ^ 1)
            rest.insert(0, z ^ 1)
        table.append([z] + rest)
    return table


def layout_of(rows, rank):
    parts = 2 if rows % 32 == 0 and rank == 128 else 1
    deep = rows // parts
    return parts, deep, (deep // 2 + 7) // 8 * 8


PLANS = {
    (2, 4): [
        ("ownz", 0, 1), ("ownp", 1), ("ownp", 0), ("ownz", 0, 2), ("ownz", 0, 3), ("zin", 0, 1),
        ("diag", 0, 0), ("ownz", 1, 1), ("zin", 0, 2), ("prep", 1), ("ownz", 1, 2), ("prep", 3),
        ("zin", 0, 3), ("diag", 0, 1), ("ownz", 1, 3), ("prep", 0), ("zin", 1, 1), ("diag", 0, 2),
        ("diag", 0, 3), ("zin", 1, 2), ("zin", 1, 3), ("diag", 1, 1), ("diag", 1, 0), ("fin", 0, 1),
        ("prep", 2), ("fin", 0, 2), ("fin", 0, 3), ("fin", 0, 0), ("diag", 1, 2), ("give", 0),
        ("diag", 1, 3), ("take", 0), ("rs1", 0, 0), ("rs1", 0, 2), ("fin", 1, 1), ("fin", 1, 2),
        ("rs1", 0, 1), ("rs1", 0, 3), ("fin", 1, 0), ("fin", 1, 3), ("give", 1), ("rs2", 0, 2),
        ("take", 1), ("sum", 0, 0), ("rs1", 1, 3), ("rs2", 0, 3), ("rs2", 0, 1), ("rs1", 1, 2),
        ("rs3", 0, 2), ("rs2", 1, 3), ("sum", 0, 1), ("rs1", 1, 1), ("rs3", 0, 3), ("rs1", 1, 0),
        ("rs2", 1, 2), ("rs3", 1, 3), ("rs2", 1, 1), ("rs2", 0, 0), ("sum", 0, 2), ("rs2", 1, 0),
        ("rs3", 0, 1), ("rs3", 1, 2), ("rs3", 1, 1), ("sum", 0, 3), ("panel", 0), ("rs3", 0, 0),
        ("rs3", 1, 0), ("collect",), ("sum", 1, 0), ("panel", 1), ("panel", 2), ("panel", 3),
        ("sum", 1, 1), ("panel", 4), ("panel", 5), ("sum", 1, 2), ("panel", 6), ("panel", 7), ("finish",),
        ("sum", 1, 3),
    ],
}


def schedule(parts, planes):
    tuned = PLANS.get((parts, planes))
    if tuned:
        return tuned
    near = range(planes)
    far = near[::-1]
    plan = []
    for h in range(parts):
        plan += [("ownp", h)] + [("ownz", h, p) for p in near[1:]]
    for h in range(parts):
        for p in near:
            plan += [("zin", h, p)] * (p > 0) + [("diag", h, p)]
    plan += [("prep", p) for p in near]
    for h in range(parts):
        plan += [("fin", h, p) for p in near] + [("give", h)]
    plan += [("take", h) for h in range(parts)] + [("sum", 0, 0)]
    for h in range(parts):
        for p in far:
            plan += [("rs1", h, p), ("rs2", h, p), ("rs3", h, p)]
    plan += [("sum", 0, 1), ("sum", 0, 2), ("collect",), ("sum", 1, 0), ("sum", 0, 3)]
    plan += [("sum", 1, 1)] + [("panel", i) for i in range(PARTS)] + [("finish",)]
    return plan + [("sum", 1, 2), ("sum", 1, 3)]

def split(v):
    hi = v.astype(BF16)
    return hi, (v - hi.astype(F32)).astype(BF16)


def thirds(v):
    a = v.astype(BF16).astype(F32)
    b = (v - a).astype(BF16).astype(F32)
    return a, b, v - a - b


def dot(a, b, dims=((1,), (0,))):
    return lax.dot_general(a, b, (dims, ((), ())), preferred_element_type=F32)


def exact(a, b, dims=((1,), (0,))):
    return lax.dot_general(
        a, b, (dims, ((), ())), precision=lax.Precision.HIGHEST, preferred_element_type=F32
    )


def kernel(grid, total_pixels, green_in, sketch_in, basis, projection, inverse_out, spec, scratch):
    C, X, Y, Z = grid
    assert C == 2
    r = scratch
    me = lax.axis_index("pix")
    c = lax.rem(me, C)
    x = lax.rem(me // C, X)
    y = lax.rem(me // (C * X), Y)
    z = me // (C * X * Y)
    green, sketch, gat, part = r["green"], r["sketch"], r["gat"], r["part"]
    rows, rank = sketch.shape
    pixels = green_in.shape[0]
    both = C * pixels
    G, deep, half = layout_of(rows, rank)
    wide = rank // G
    slab = X * Y * C * rows
    table = order_of(Z)
    mine = pl.ds(pl.multiple_of(c * pixels, 8), pixels)
    low, high = pl.ds(0, half), pl.ds(half, deep - half)
    spans = (low, high)

    def dev(zz, yy, xx, cc):
        return (((zz * Y + yy) * X + xx) * C + cc,)

    def at(v, d, n):
        return lax.rem(v + d + n, n)

    def near(p):
        out = table[0][p]
        for k in range(1, Z):
            out = jnp.where(z == k, table[k][p], out)
        return out

    partner = dev(z, y, x, 1 - c)
    dxs, dys = range(1, X), range(1, Y)
    counter = [0]
    sends = []

    sent = [0]

    def copy(src, dst, recv, to, leaves=None):
        pltpu.make_async_remote_copy(
            src_ref=src, dst_ref=dst, send_sem=r["send"].at[0] if leaves is None else leaves, recv_sem=recv,
            device_id=to, device_id_type=MESH,
        ).start()
        if leaves is None:
            sent[0] += math.prod(src.shape) // rank

    def tally(count, leaves):
        ref = r["tally"].at[pl.ds(0, count)]
        return pltpu.make_async_remote_copy(
            src_ref=ref, dst_ref=ref, send_sem=leaves, recv_sem=leaves,
            device_id=partner, device_id_type=MESH,
        )

    def arrive(recv, count):
        ref = r["tally"].at[pl.ds(0, count)]
        pltpu.make_async_remote_copy(
            src_ref=ref, dst_ref=ref, send_sem=r["send"].at[0], recv_sem=recv,
            device_id=partner, device_id_type=MESH,
        ).wait_recv()

    def finish_sends():
        tally(sent[0], r["send"].at[0]).wait_send()
        drain_gram()
        drain_spectrum()

    load_sketch = pltpu.make_async_copy(sketch_in, sketch, r["load"].at[0])
    load_green = pltpu.make_async_copy(green_in, green.at[mine], r["load"].at[1])
    load_sketch.start()
    load_green.start()
    barrier = pltpu.get_barrier_semaphore()
    peers = [(partner, None)]
    peers += [(dev(z, y, at(x, dx, X), c), None) for dx in dxs]
    peers += [(dev(z, at(y, dy, Y), x, c), None) for dy in dys]
    peers += [(dev(z - 1, y, x, c), z > 0), (dev(z + 1, y, x, c), z < Z - 1)]

    def greet(peer):
        pl.semaphore_signal(barrier, inc=1, device_id=peer, device_id_type=MESH)

    for peer, when in peers:
        if when is None:
            greet(peer)
        else:
            pl.when(when)(functools.partial(greet, peer))
    lanes = lax.broadcasted_iota(jnp.int32, (deep, rank), 1)
    load_sketch.wait()
    if G == 1:
        gat[0, z, y, x] = sketch[...]
    else:
        top, bottom = sketch[:deep], sketch[deep:]
        gat[0, z, y, x] = jnp.where(lanes < wide, top, pltpu.roll(bottom, wide, 1))
        gat[1, z, y, x] = jnp.where(lanes < wide, pltpu.roll(top, wide, 1), bottom)
    known = len(peers) - 2 + jnp.where(z > 0, 1, 0) + jnp.where(z < Z - 1, 1, 0)
    pl.semaphore_wait(barrier, known)

    rest = deep - half

    def along_x(h, s, k):
        ref = gat.at[h, near(s), y, x, spans[k]]
        for dx in dxs:
            copy(ref, ref, r["agr" if k else "agf"].at[h, s], dev(z, y, at(x, dx, X), c))

    def along_y(h, s, k):
        ref = gat.at[h, near(s), y, x, spans[k]]
        for dy in dys:
            copy(ref, ref, r["agf" if k else "agr"].at[h, s], dev(z, at(y, dy, Y), x, c))

    def in_plane(h, s):
        along_x(h, s, 0)
        along_y(h, s, 1)
        along_x(h, s, 1)
        along_y(h, s, 0)

    def tell(sem, to):
        pl.semaphore_signal(sem, inc=1, device_id=to, device_id_type=MESH)

    def learn(j):
        up, down = r["kup"].at[j], r["kdown"].at[j]
        pl.when((z >= 1) & (z + j < Z))(functools.partial(tell, up, dev(z - 1, y, x, c)))
        pl.when((z + 1 < Z) & (z - j >= 0))(functools.partial(tell, down, dev(z + 1, y, x, c)))

    def known_far(j):
        pl.when(z + 1 + j < Z)(lambda: pl.semaphore_wait(r["kup"].at[j], 1))
        pl.when(z - 1 - j >= 0)(lambda: pl.semaphore_wait(r["kdown"].at[j], 1))

    reach = [0]

    def to_plane(h, p):
        far = max(abs(row[p] - row[0]) for row in table)
        while reach[0] < far - 1:
            reach[0] += 1
            learn(reach[0])
            known_far(reach[0])
        ref = gat.at[h, z, y, x]
        copy(ref, ref, r["agz"].at[h, z], dev(near(p), y, x, c))

    def zin(h, s):
        arrive(r["agz"].at[h, near(s)], deep)
        in_plane(h, s)

    def diag(h, s):
        zc = near(s)
        if dxs or dys:
            arrive(r["agf"].at[h, s], len(dxs) * half + len(dys) * rest)
        for dx in dxs:
            for dy in dys:
                ref = gat.at[h, zc, y, at(x, -dx, X), low]
                copy(ref, ref, r["agr"].at[h, s], dev(z, at(y, dy, Y), x, c))
        for dy in dys:
            for dx in dxs:
                ref = gat.at[h, zc, at(y, -dy, Y), x, high]
                copy(ref, ref, r["agr"].at[h, s], dev(z, y, at(x, dx, X), c))

    def swap():
        pltpu.make_async_remote_copy(
            src_ref=green_in, dst_ref=green.at[mine], send_sem=r["swap_send"].at[0], recv_sem=r["swap"].at[0],
            device_id=partner, device_id_type=MESH,
        ).start()

    def swapped():
        other = green.at[pl.ds(pl.multiple_of((1 - c) * pixels, 8), pixels)]
        load_green.wait()
        pltpu.make_async_remote_copy(
            src_ref=green_in, dst_ref=other, send_sem=r["swap_send"].at[0], recv_sem=r["swap"].at[0],
            device_id=partner, device_id_type=MESH,
        ).wait()

    gl, gt, turned = r["gl"], r["gt"], r["turned"]

    def prep(s):
        g = green[:, pl.ds(pl.multiple_of(near(s) * slab, 128), slab)]
        turned[...] = g.T
        for w in range(X * Y):
            block = turned[pl.ds(pl.multiple_of(w * C * rows + c * rows, 8), rows)]
            hi, lo = split(block)
            gt[s, w] = jnp.concatenate(
                [v[g * deep : (g + 1) * deep] for g in range(G) for v in (hi, lo)], axis=1
            )
            halves = [split(block[g * deep : (g + 1) * deep].T) for g in range(G)]
            gl[s, w] = jnp.concatenate([v[0] for v in halves] + [v[1] for v in halves], axis=0)

    started = set()

    def multiply(h, s):
        if dxs or dys:
            arrive(r["agr"].at[h, s], len(dxs) * rest + len(dys) * half + len(dxs) * len(dys) * deep)
        zc = near(s)
        out = None
        for w in range(X * Y):
            b_hi, b_lo = split(gat[h, zc, w // X, w % X])
            tall = dot(gl[s, w], b_hi)
            term = tall[: G * both] + tall[G * both :] + dot(gl[s, w, : G * both], b_lo)
            out = term if out is None else out + term
        if h in started:
            r["acc"][h] += out
        else:
            started.add(h)
            r["acc"][h] = out

    lane_b = lax.broadcasted_iota(jnp.int32, (both, rank), 1)

    def give(h):
        v = r["acc"][h]
        if G == 2:
            v = jnp.where(lane_b < wide, v[:both], v[both:])
        r["mine"][h] = v
        copy(r["mine"].at[h], r["theirs"].at[h], r["swap"].at[1 + h], partner)

    weights = {}

    def take(h):
        arrive(r["swap"].at[1 + h], both)
        v = r["mine"][h] + r["theirs"][h]
        if G == 2:
            v = v + pltpu.roll(v, wide, 1)
        r["folded"][h] = v
        tall = [v] if G == 1 else [jnp.where(lane_b < wide, v, 0.0), jnp.where(lane_b < wide, 0.0, v)]
        pairs = [split(t) for t in tall]
        for i in range(2):
            r["weights"][h, i] = jnp.concatenate([p[i] for p in pairs for _ in range(2)], axis=0)

    def merge():
        if G == 1:
            r["sketched"][...] = r["folded"][0]
        else:
            r["sketched"][...] = jnp.where(lane_b < wide, r["folded"][0], r["folded"][1])

    owner = C - 1
    owns = c == owner
    here = y * X + x
    q = rank // (X * Y)
    spots = [(dy, dx) for dy in range(Y) for dx in range(X)]
    n = len(spots)

    def total_sum(k, value, per_chip):
        src, inc, top, res = (r[n].at[k] for n in ("t_src", "t_in", "t_top", "t_res"))
        leaves = r["sums_send"].at[k]

        def send(ref, dst, step, to):
            copy(ref, dst, r["sums"].at[k, step], to, leaves)

        def scatter(skip):
            for dy, dx in spots[skip:]:
                yy, xx = at(y, dy, Y), at(x, dx, X)
                send(src.at[yy * X + xx], inc.at[c, dy * X + dx], 0, dev(z, yy, xx, owner))

        def step0():
            def fill():
                v = value()
                for w in range(n):
                    src[w] = v[w * q : (w + 1) * q]

            if per_chip:
                @pl.when(owns)
                def _():
                    fill()
                    scatter(1)
            else:
                fill()
                pl.when(owns)(lambda: scatter(1))
                pl.when(~owns)(lambda: scatter(0))

        def step1():
            @pl.when(owns)
            def _():
                total = src[here]
                arrive(r["sums"].at[k, 0], (n - 1 if per_chip else 2 * n - 1) * q)
                for i in range(n):
                    if i:
                        total = total + inc[owner, i]
                    if not per_chip:
                        total = total + inc[0, i]
                top[z] = total
                for p in range(1, Z):
                    send(top.at[z], top.at[z], 1, dev(near(p), y, x, owner))

        def step2():
            @pl.when(owns)
            def _():
                if Z > 1:
                    arrive(r["sums"].at[k, 1], (Z - 1) * q)
                res[here] = jnp.sum(top[...], axis=0)
                for dy, dx in spots[::-1]:
                    yy, xx = at(y, dy, Y), at(x, dx, X)
                    for cc in range(C):
                        if (dy, dx) != (0, 0) or cc != owner:
                            send(res.at[here], res.at[here], 2, dev(z, yy, xx, cc))

        def step3():
            pl.when(~owns)(lambda: arrive(r["sums"].at[k, 2], n * q))
            if n > 1:
                pl.when(owns)(lambda: arrive(r["sums"].at[k, 2], (n - 1) * q))

        def drain():
            pl.when(owns)(lambda: tally((n - 1 + Z - 1 + 2 * n - 1) * q, leaves).wait_send())
            if not per_chip:
                pl.when(~owns)(lambda: tally(n * q, leaves).wait_send())

        def total():
            return jnp.concatenate([res[w] for w in range(n)], axis=0)

        return [step0, step1, step2, step3], total, drain

    def rs1(h, s):
        for w in range(X * Y):
            part[h, s, w // X, w % X] = dot(gt[s, w], r["weights"][h, 0]) + dot(gt[s, w], r["weights"][h, 1])
        for dy in dys:
            for dx in dxs:
                yy, xx = at(y, dy, Y), at(x, dx, X)
                copy(part.at[h, s, yy, xx, low], r["rda"].at[h, s, dy, dx], r["rsf"].at[h, s],
                     dev(z, yy, x, c))
                copy(part.at[h, s, yy, xx, high], r["rdb"].at[h, s, dy, dx], r["rsf"].at[h, s],
                     dev(z, y, xx, c))
        for dy in dys:
            yy = at(y, dy, Y)
            copy(part.at[h, s, yy, x, low], r["rya"].at[h, s, dy], r["rsr"].at[h, s], dev(z, yy, x, c))
        for dx in dxs:
            xx = at(x, dx, X)
            copy(part.at[h, s, y, xx, high], r["rxb"].at[h, s, dx], r["rsr"].at[h, s], dev(z, y, xx, c))

    def rs2(h, s):
        if dxs and dys:
            arrive(r["rsf"].at[h, s], len(dxs) * len(dys) * deep)
        for dx in dxs:
            xx = at(x, dx, X)
            ref = part.at[h, s, y, xx, low]
            total = ref[...]
            for dy in dys:
                total = total + r["rda"][h, s, dy, dx]
            ref[...] = total
            copy(ref, r["rxa"].at[h, s, dx], r["rsr"].at[h, s], dev(z, y, xx, c))
        for dy in dys:
            yy = at(y, dy, Y)
            ref = part.at[h, s, yy, x, high]
            total = ref[...]
            for dx in dxs:
                total = total + r["rdb"][h, s, dy, dx]
            ref[...] = total
            copy(ref, r["ryb"].at[h, s, dy], r["rsr"].at[h, s], dev(z, yy, x, c))

    fin = r["fin"]

    def rs3(h, s):
        if dxs or dys:
            arrive(r["rsr"].at[h, s], (len(dxs) + len(dys)) * deep)
        total = part[h, s, y, x, low]
        for name, ds in (("rya", dys), ("rxa", dxs)):
            for d in ds:
                total = total + r[name][h, s, d]
        fin[h, s, low] = total
        total = part[h, s, y, x, high]
        for name, ds in (("rxb", dxs), ("ryb", dys)):
            for d in ds:
                total = total + r[name][h, s, d]
        fin[h, s, high] = total
        if s:
            copy(fin.at[h, s], r["rz"].at[h, z], r["rsz"].at[h], dev(near(s), y, x, c))

    def collect():
        got = []
        for h in range(G):
            total = fin[h, 0]
            if Z > 1:
                arrive(r["rsz"].at[h], (Z - 1) * deep)
            for p in range(1, Z):
                total = total + r["rz"][h, near(p)]
            got.append(total)
        if G == 1:
            r["raw"][...] = got[0]
        else:
            r["raw"][:deep] = jnp.where(lanes < wide, got[0], pltpu.roll(got[1], wide, 1))
            r["raw"][deep:] = jnp.where(lanes < wide, pltpu.roll(got[0], wide, 1), got[1])

    aug = r["aug"]
    lane = lax.broadcasted_iota(jnp.int32, (rank, rank), 1)
    row_of = lax.broadcasted_iota(jnp.int32, (rank, rank), 0)

    def eliminate(p, _):
        first = pl.multiple_of(p * PANEL, PANEL)
        lanes = lane[:PANEL]
        index = row_of[:PANEL, :1]
        block = aug[pl.ds(first, PANEL), :]
        left = block[:, :rank]
        cols = [
            jnp.sum(jnp.where(lanes == first + k, left, 0.0), axis=1, keepdims=True)
            for k in range(PANEL)
        ]
        scale = jnp.zeros((PANEL, 1), F32)
        for k in range(PANEL):
            inv = 1.0 / cols[k][k : k + 1]
            f = jnp.where(index > k, cols[k] * inv, 0.0)
            for m in range(k + 1, PANEL):
                cols[m] = cols[m] - f * cols[m][k : k + 1]
            block = block - f * block[k : k + 1]
            scale = jnp.where(index == k, inv, scale)
        u = thirds(jnp.where(lanes >= first + PANEL, block[:, :rank] * scale, 0.0))
        v = thirds(block)
        lhs = jnp.concatenate([u[i] for i in (0, 0, 0, 1, 1, 2)], axis=0).astype(BF16)
        rhs = jnp.concatenate([v[i] for i in (0, 1, 2, 0, 1, 0)], axis=0).astype(BF16)
        aug[...] = aug[...] - dot(lhs, rhs, ((0,), (0,)))
        aug[pl.ds(first, PANEL), :] = block
        return 0

    def begin():
        aug[:, :rank] = gram_total()
        aug[:, rank:] = jnp.where(lane == row_of, 1.0, 0.0)

    def chol(first, last):
        lax.fori_loop(first, last, eliminate, 0)

    def finish():
        diag = jnp.sum(jnp.where(lane == row_of, aug[:, :rank], 0.0), axis=1, keepdims=True)
        inverse = aug[:, rank:] * lax.rsqrt(diag)
        inverse_out[...] = inverse
        basis[...] = jnp.sqrt(F32(total_pixels)) * exact(r["sketched"][mine], inverse, ((1,), (1,)))
        projection[...] = exact(r["raw"][...], inverse, ((1,), (1,)))

    def gram_part():
        v = r["sketched"][...]
        return exact(v, v, ((0,), (0,)))

    def raw_part():
        v = r["raw"][...]
        return exact(v, v, ((0,), (0,)))

    gram, gram_total, drain_gram = total_sum(0, gram_part, True)
    spectrum, spectrum_total, drain_spectrum = total_sum(1, raw_part, False)
    panels = rank // PANEL

    def panel(i):
        if i == 0:
            begin()
        chol(panels * i // PARTS, panels * (i + 1) // PARTS)

    def send_own(h):
        in_plane(h, 0)
        if h == 0:
            swap()

    def give_take(h):
        take(h)
        if h == G - 1:
            merge()

    def prepare(s):
        if not prepared:
            swapped()
        prepared.add(s)
        prep(s)

    prepared = set()
    steps = dict(
        ownp=send_own, ownz=to_plane, prep=prepare, zin=zin, diag=diag, fin=multiply, give=give,
        take=give_take, rs1=rs1, rs2=rs2, rs3=rs3, collect=collect, sum=lambda k, i: (gram, spectrum)[k][i](),
        panel=panel, finish=finish,
    )
    for name, *index in schedule(G, Z):
        steps[name](*index)
    spec[...] = spectrum_total()
    finish_sends()


def finish_kernel(patches, basis_in, projection_in, inverse_in, spec_in, basis, projection, spectrum):
    inverse = inverse_in[...]
    basis[...] = basis_in[...]
    projection[...] = projection_in[...]
    spectrum[...] = exact(exact(inverse, spec_in[...]), inverse, ((1,), (1,))) / F32(patches)


def body(grid, green, sketch):
    C, X, Y, Z = grid
    rows, rank = sketch.shape
    pixels, patches = green.shape
    G, deep, half = layout_of(rows, rank)
    other = deep - half
    both = C * pixels
    few = rank // (X * Y)

    def vmem(*shape):
        return pltpu.VMEM(shape, F32)

    def packed(*shape):
        return pltpu.VMEM(shape, BF16)

    def dma(*shape):
        return pltpu.SemaphoreType.DMA(shape)

    flags = pltpu.SemaphoreType.REGULAR((Z,))
    links = X - 1 + Y - 1 + (X - 1) * (Y - 1)
    count = 2 * G * deep * (Z * links + Z - 1) + G * both
    scratch = dict(
        green=vmem(both, patches), sketch=vmem(rows, rank), gat=vmem(G, Z, Y, X, deep, rank),
        turned=vmem(X * Y * C * rows, both),
        gl=packed(Z, X * Y, 2 * G * both, deep), gt=packed(Z, X * Y, deep, 2 * G * both),
        acc=vmem(G, G * both, rank), mine=vmem(G, both, rank), theirs=vmem(G, both, rank),
        folded=vmem(G, both, rank), weights=packed(G, 2, 2 * G * both, rank), sketched=vmem(both, rank),
        part=vmem(G, Z, Y, X, deep, rank),
        rda=vmem(G, Z, Y, X, half, rank), rdb=vmem(G, Z, Y, X, other, rank),
        rya=vmem(G, Z, Y, half, rank), rxb=vmem(G, Z, X, other, rank),
        rxa=vmem(G, Z, X, half, rank), ryb=vmem(G, Z, Y, other, rank),
        fin=vmem(G, Z, deep, rank), rz=vmem(G, Z, deep, rank), raw=vmem(rows, rank),
        t_src=vmem(2, X * Y, few, rank), t_in=vmem(2, C, X * Y, few, rank),
        t_top=vmem(2, Z, few, rank), t_res=vmem(2, X * Y, few, rank),
        aug=vmem(rank, 2 * rank), kup=flags, kdown=flags,
        tally=vmem(count, rank),
        send=dma(1), load=dma(2), swap=dma(1 + G), swap_send=dma(1),
        agz=dma(G, Z), agf=dma(G, Z), agr=dma(G, Z),
        rsf=dma(G, Z), rsr=dma(G, Z), rsz=dma(G), sums=dma(2, 3), sums_send=dma(2),
    )
    total_pixels = pixels * C * X * Y * Z
    tall = jax.ShapeDtypeStruct((pixels, rank), F32)
    wide = jax.ShapeDtypeStruct((rows, rank), F32)
    square = jax.ShapeDtypeStruct((rank, rank), F32)
    whole = pl.BlockSpec(memory_space=pltpu.VMEM)
    parts = pl.pallas_call(
        functools.partial(kernel, grid, total_pixels),
        out_shape=(tall, wide, square, square),
        in_specs=[pl.BlockSpec(memory_space=pl.ANY)] * 2,
        out_specs=(whole,) * 4,
        scratch_shapes=[scratch],
        compiler_params=pltpu.CompilerParams(
            collective_id=0, has_side_effects=True, vmem_limit_bytes=63 * 1024 * 1024
        ),
    )(green, sketch)
    return pl.pallas_call(
        functools.partial(finish_kernel, patches),
        out_shape=(tall, wide, square),
        in_specs=[whole] * 4,
        out_specs=(whole,) * 3,
    )(*parts)


def solution(mesh):
    grid = grid_of(mesh.shape["pix"])
    in_specs = (P("pix", None), P("pix", None))
    out_specs = (P("pix", None), P("pix", None), P())
    return jax.shard_map(
        functools.partial(body, grid), mesh=mesh, in_specs=in_specs, out_specs=out_specs, check_vma=False
    )
```

```python
import functools
import math

import jax
import jax.numpy as jnp
from jax import lax
from jax.experimental import pallas as pl
from jax.experimental.pallas import tpu as pltpu
from jax.sharding import PartitionSpec as P

MESH = pl.DeviceIdType.MESH
F32 = jnp.float32
BF16 = jnp.bfloat16
PANEL = 8
PARTS = 8
VLIM = 53.63
KEEP = 6


def grid_of(devices):
    cores = 2 if devices % 2 == 0 else 1
    chips = devices // cores
    side = 1
    for k in range(1, chips + 1):
        if chips % (k * k) == 0 and k * k * k <= chips:
            side = k
    return cores, side, side, chips // (side * side)


def order_of(planes):
    table = []
    for z in range(planes):
        rest = sorted((k for k in range(planes) if k != z), key=lambda k: (abs(k - z), k))
        if planes % 2 == 0:
            rest.remove(z ^ 1)
            rest.insert(0, z ^ 1)
        table.append([z] + rest)
    return table


def layout_of(grid, rows, rank):
    C, X, Y, Z = grid
    parts = 2 if rows % 32 == 0 and rank == 128 else 1
    deep = rows // parts
    half = (deep // 2 + 7) // 8 * 8
    keep = min(max(8, KEEP * half // 6 // 8 * 8), deep - half)
    return parts, deep, half, keep if Z % 2 == 0 and X * Y > 1 and 0 < keep < half else None


PLANS = {
    (2, 4): [
        ("ownz", 0, 1), ("ownz", 1, 1), ("ownp", 1), ("ownz", 0, 2), ("ownp", 0), ("ownz", 0, 3),
        ("diag", 1, 0), ("zin", 0, 1), ("prep", 1), ("prep", 0), ("diag", 0, 0), ("zin", 0, 2),
        ("ownz", 1, 2), ("ownz", 1, 3), ("prep", 2), ("zin", 0, 3), ("diag", 0, 1), ("zin", 1, 1),
        ("diag", 0, 2), ("fin", 0, 0), ("diag", 0, 3), ("fin", 1, 0), ("zin", 1, 2), ("prep", 3),
        ("zin", 1, 3), ("fin", 0, 1), ("fin", 0, 2), ("diag", 1, 1), ("fin", 0, 3), ("give", 0),
        ("diag", 1, 2), ("take", 0), ("diag", 1, 3), ("rs1", 0, 3), ("rs1", 0, 2), ("fin", 1, 1),
        ("rs1", 0, 1), ("fin", 1, 2), ("rs1", 0, 0), ("fin", 1, 3), ("rs2", 0, 3), ("give", 1),
        ("rs2", 0, 2), ("take", 1), ("rs1", 1, 3), ("sum", 0, 0), ("rs1", 1, 2), ("rs2", 0, 1),
        ("rs3", 0, 3), ("rs3", 0, 2), ("rs2", 1, 3), ("rs1", 1, 1), ("rs2", 1, 2), ("sum", 0, 1),
        ("rs1", 1, 0), ("rs3", 0, 1), ("rs3", 1, 3), ("rs2", 1, 1), ("rs2", 0, 0), ("rs3", 1, 2),
        ("sum", 0, 2), ("rs2", 1, 0), ("rs3", 1, 1), ("rs3", 0, 0), ("sum", 0, 3), ("rs3", 1, 0),
        ("collect",), ("sum", 1, 0), ("panel", 0), ("panel", 1), ("panel", 2), ("sum", 1, 1), ("panel", 3),
        ("panel", 4), ("sum", 1, 2), ("panel", 5), ("panel", 6), ("panel", 7), ("finish",), ("sum", 1, 3),
    ],
}


def schedule(parts, planes):
    tuned = PLANS.get((parts, planes))
    if tuned:
        return tuned
    near = range(planes)
    far = near[::-1]
    plan = []
    for h in range(parts):
        plan += [("ownp", h)] + [("ownz", h, p) for p in near[1:]]
    for h in range(parts):
        for p in near:
            plan += [("zin", h, p)] * (p > 0) + [("diag", h, p)]
    plan += [("prep", p) for p in near] + [("share", h) for h in range(parts)]
    for h in range(parts):
        plan += [("fin", h, p) for p in near] + [("give", h)]
    plan += [("take", h) for h in range(parts)] + [("sum", 0, 0)]
    for h in range(parts):
        for p in far:
            plan += [("rs1", h, p), ("rs2", h, p), ("rs3", h, p)]
    plan += [("sum", 0, 1), ("sum", 0, 2), ("collect",), ("sum", 1, 0), ("sum", 0, 3)]
    plan += [("sum", 1, 1)] + [("panel", i) for i in range(PARTS)] + [("finish",)]
    return plan + [("sum", 1, 2), ("sum", 1, 3)]

def split(v):
    hi = v.astype(BF16)
    return hi, (v - hi.astype(F32)).astype(BF16)


def thirds(v):
    a = v.astype(BF16).astype(F32)
    b = (v - a).astype(BF16).astype(F32)
    return a, b, v - a - b


def dot(a, b, dims=((1,), (0,))):
    return lax.dot_general(a, b, (dims, ((), ())), preferred_element_type=F32)


def exact(a, b, dims=((1,), (0,))):
    return lax.dot_general(
        a, b, (dims, ((), ())), precision=lax.Precision.HIGHEST, preferred_element_type=F32
    )


def kernel(grid, total_pixels, green_in, sketch_in, basis, projection, inverse_out, spec, scratch):
    C, X, Y, Z = grid
    assert C == 2
    r = scratch
    me = lax.axis_index("pix")
    c = lax.rem(me, C)
    x = lax.rem(me // C, X)
    y = lax.rem(me // (C * X), Y)
    z = me // (C * X * Y)
    green, sketch, gat, part = r["green"], r["sketch"], r["gat"], r["part"]
    rows, rank = sketch.shape
    pixels = green_in.shape[0]
    both = C * pixels
    G, deep, half, keep = layout_of(grid, rows, rank)
    wide = rank // G
    slab = X * Y * C * rows
    table = order_of(Z)
    mine = pl.ds(pl.multiple_of(c * pixels, 8), pixels)
    rest = deep - half
    other_rows = [(dy, dx) for dy in range(Y) for dx in range(X) if (dy, dx) != (0, 0)]
    middle = pl.ds(keep or 0, deep - 2 * (keep or 0))

    def low(s):
        return pl.ds(0, half if keep is None or s != 1 else keep)

    def high(s):
        return pl.ds(half, rest) if keep is None or s != 1 else pl.ds(deep - keep, keep)

    def n_low(s):
        return low(s).size

    def n_high(s):
        return high(s).size


    def dev(zz, yy, xx, cc):
        return (((zz * Y + yy) * X + xx) * C + cc,)

    def at(v, d, n):
        return lax.rem(v + d + n, n)

    def near(p):
        out = table[0][p]
        for k in range(1, Z):
            out = jnp.where(z == k, table[k][p], out)
        return out

    partner = dev(z, y, x, 1 - c)
    dxs, dys = range(1, X), range(1, Y)
    counter = [0]
    sends = []

    sent = [0]

    def copy(src, dst, recv, to, leaves=None):
        pltpu.make_async_remote_copy(
            src_ref=src, dst_ref=dst, send_sem=r["send"].at[0] if leaves is None else leaves, recv_sem=recv,
            device_id=to, device_id_type=MESH,
        ).start()
        if leaves is None:
            sent[0] += math.prod(src.shape) // rank

    def tally(count, leaves):
        ref = r["tally"].at[pl.ds(0, count)]
        return pltpu.make_async_remote_copy(
            src_ref=ref, dst_ref=ref, send_sem=leaves, recv_sem=leaves,
            device_id=partner, device_id_type=MESH,
        )

    def arrive(recv, count):
        ref = r["tally"].at[pl.ds(0, count)]
        pltpu.make_async_remote_copy(
            src_ref=ref, dst_ref=ref, send_sem=r["send"].at[0], recv_sem=recv,
            device_id=partner, device_id_type=MESH,
        ).wait_recv()

    def finish_sends():
        tally(sent[0], r["send"].at[0]).wait_send()
        drain_gram()
        drain_spectrum()

    load_sketch = pltpu.make_async_copy(sketch_in, sketch, r["load"].at[0])
    load_green = pltpu.make_async_copy(green_in, green.at[mine], r["load"].at[1])
    load_sketch.start()
    load_green.start()
    barrier = pltpu.get_barrier_semaphore()
    peers = [(partner, None)]
    peers += [(dev(z, y, at(x, dx, X), c), None) for dx in dxs]
    peers += [(dev(z, at(y, dy, Y), x, c), None) for dy in dys]
    peers += [(dev(z - 1, y, x, c), z > 0), (dev(z + 1, y, x, c), z < Z - 1)]

    def greet(peer):
        pl.semaphore_signal(barrier, inc=1, device_id=peer, device_id_type=MESH)

    for peer, when in peers:
        if when is None:
            greet(peer)
        else:
            pl.when(when)(functools.partial(greet, peer))
    lanes = lax.broadcasted_iota(jnp.int32, (deep, rank), 1)
    load_sketch.wait()
    if G == 1:
        gat[0, z, y, x] = sketch[...]
    else:
        top, bottom = sketch[:deep], sketch[deep:]
        gat[0, z, y, x] = jnp.where(lanes < wide, top, pltpu.roll(bottom, wide, 1))
        gat[1, z, y, x] = jnp.where(lanes < wide, pltpu.roll(top, wide, 1), bottom)
    known = len(peers) - 2 + jnp.where(z > 0, 1, 0) + jnp.where(z < Z - 1, 1, 0)
    pl.semaphore_wait(barrier, known)

    def along_x(h, s, k):
        ref = gat.at[h, near(s), y, x, (low, high)[k](s)]
        for dx in dxs:
            copy(ref, ref, r["agr" if k else "agf"].at[h, s], dev(z, y, at(x, dx, X), c))

    def along_y(h, s, k):
        ref = gat.at[h, near(s), y, x, (low, high)[k](s)]
        for dy in dys:
            copy(ref, ref, r["agf" if k else "agr"].at[h, s], dev(z, at(y, dy, Y), x, c))

    def in_plane(h, s):
        along_x(h, s, 0)
        along_y(h, s, 1)
        along_x(h, s, 1)
        along_y(h, s, 0)

    def tell(sem, to):
        pl.semaphore_signal(sem, inc=1, device_id=to, device_id_type=MESH)

    def learn(j):
        up, down = r["kup"].at[j], r["kdown"].at[j]
        pl.when((z >= 1) & (z + j < Z))(functools.partial(tell, up, dev(z - 1, y, x, c)))
        pl.when((z + 1 < Z) & (z - j >= 0))(functools.partial(tell, down, dev(z + 1, y, x, c)))

    def known_far(j):
        pl.when(z + 1 + j < Z)(lambda: pl.semaphore_wait(r["kup"].at[j], 1))
        pl.when(z - 1 - j >= 0)(lambda: pl.semaphore_wait(r["kdown"].at[j], 1))

    reach = [0]

    def to_plane(h, p):
        far = max(abs(row[p] - row[0]) for row in table)
        while reach[0] < far - 1:
            reach[0] += 1
            learn(reach[0])
            known_far(reach[0])
        ref = gat.at[h, z, y, x]
        copy(ref, ref, r["agz"].at[h, z], dev(near(p), y, x, c))

    def zin(h, s):
        arrive(r["agz"].at[h, near(s)], deep)
        in_plane(h, s)

    def diag(h, s):
        zc = near(s)
        if dxs or dys:
            arrive(r["agf"].at[h, s], len(dxs) * n_low(s) + len(dys) * n_high(s))
        for dx in dxs:
            for dy in dys:
                ref = gat.at[h, zc, y, at(x, -dx, X), low(s)]
                copy(ref, ref, r["agr"].at[h, s], dev(z, at(y, dy, Y), x, c))
        for dy in dys:
            for dx in dxs:
                ref = gat.at[h, zc, at(y, -dy, Y), x, high(s)]
                copy(ref, ref, r["agr"].at[h, s], dev(z, y, at(x, dx, X), c))

    def swap():
        pltpu.make_async_remote_copy(
            src_ref=green_in, dst_ref=green.at[mine], send_sem=r["swap_send"].at[0], recv_sem=r["swap"].at[0],
            device_id=partner, device_id_type=MESH,
        ).start()

    def swapped():
        other = green.at[pl.ds(pl.multiple_of((1 - c) * pixels, 8), pixels)]
        load_green.wait()
        pltpu.make_async_remote_copy(
            src_ref=green_in, dst_ref=other, send_sem=r["swap_send"].at[0], recv_sem=r["swap"].at[0],
            device_id=partner, device_id_type=MESH,
        ).wait()

    gl, gt, turned = r["gl"], r["gt"], r["turned"]

    def prep(s):
        g = green[:, pl.ds(pl.multiple_of(near(s) * slab, 128), slab)]
        turned[...] = g.T
        for w in range(X * Y):
            block = turned[pl.ds(pl.multiple_of(w * C * rows + c * rows, 8), rows)]
            hi, lo = split(block)
            gt[s, w] = jnp.concatenate(
                [v[g * deep : (g + 1) * deep] for g in range(G) for v in (hi, lo)], axis=1
            )
            halves = [split(block[g * deep : (g + 1) * deep].T) for g in range(G)]
            gl[s, w] = jnp.concatenate([v[0] for v in halves] + [v[1] for v in halves], axis=0)

    started = set()

    gathered = set()

    def in_hand(h, s):
        if (dxs or dys) and (h, s) not in gathered:
            gathered.add((h, s))
            diags = len(dxs) * len(dys)
            count = (len(dxs) + diags) * n_high(s) + (len(dys) + diags) * n_low(s)
            arrive(r["agr"].at[h, s], count)

    def share(h):
        if keep is not None:
            in_hand(h, 0)
            for dy, dx in other_rows:
                ref = gat.at[h, z, at(y, dy, Y), at(x, dx, X), middle]
                copy(ref, ref, r["age"].at[h], dev(near(1), y, x, c))

    def multiply(h, s):
        in_hand(h, s)
        if s == 1 and keep is not None:
            arrive(r["age"].at[h], len(other_rows) * middle.size)
        zc = near(s)
        out = None
        for w in range(X * Y):
            b_hi, b_lo = split(gat[h, zc, w // X, w % X])
            tall = dot(gl[s, w], b_hi)
            term = tall[: G * both] + tall[G * both :] + dot(gl[s, w, : G * both], b_lo)
            out = term if out is None else out + term
        if h in started:
            r["acc"][h] += out
        else:
            started.add(h)
            r["acc"][h] = out

    lane_b = lax.broadcasted_iota(jnp.int32, (both, rank), 1)

    def give(h):
        v = r["acc"][h]
        if G == 2:
            v = jnp.where(lane_b < wide, v[:both], v[both:])
        r["mine"][h] = v
        copy(r["mine"].at[h], r["theirs"].at[h], r["swap"].at[1 + h], partner)

    weights = {}

    def take(h):
        arrive(r["swap"].at[1 + h], both)
        v = r["mine"][h] + r["theirs"][h]
        if G == 2:
            v = v + pltpu.roll(v, wide, 1)
        r["folded"][h] = v
        tall = [v] if G == 1 else [jnp.where(lane_b < wide, v, 0.0), jnp.where(lane_b < wide, 0.0, v)]
        pairs = [split(t) for t in tall]
        for i in range(2):
            r["weights"][h, i] = jnp.concatenate([p[i] for p in pairs for _ in range(2)], axis=0)

    def merge():
        if G == 1:
            r["sketched"][...] = r["folded"][0]
        else:
            r["sketched"][...] = jnp.where(lane_b < wide, r["folded"][0], r["folded"][1])

    owner = C - 1
    owns = c == owner
    here = y * X + x
    q = rank // (X * Y)
    spots = [(dy, dx) for dy in range(Y) for dx in range(X)]
    n = len(spots)

    def total_sum(k, value, per_chip):
        src, inc, top, res = (r[n].at[k] for n in ("t_src", "t_in", "t_top", "t_res"))
        leaves = r["sums_send"].at[k]

        def send(ref, dst, step, to):
            copy(ref, dst, r["sums"].at[k, step], to, leaves)

        def scatter(skip):
            for dy, dx in spots[skip:]:
                yy, xx = at(y, dy, Y), at(x, dx, X)
                send(src.at[yy * X + xx], inc.at[c, dy * X + dx], 0, dev(z, yy, xx, owner))

        def step0():
            def fill():
                v = value()
                for w in range(n):
                    src[w] = v[w * q : (w + 1) * q]

            if per_chip:
                @pl.when(owns)
                def _():
                    fill()
                    scatter(1)
            else:
                fill()
                pl.when(owns)(lambda: scatter(1))
                pl.when(~owns)(lambda: scatter(0))

        def step1():
            @pl.when(owns)
            def _():
                total = src[here]
                arrive(r["sums"].at[k, 0], (n - 1 if per_chip else 2 * n - 1) * q)
                for i in range(n):
                    if i:
                        total = total + inc[owner, i]
                    if not per_chip:
                        total = total + inc[0, i]
                top[z] = total
                for p in range(1, Z):
                    send(top.at[z], top.at[z], 1, dev(near(p), y, x, owner))

        def step2():
            @pl.when(owns)
            def _():
                if Z > 1:
                    arrive(r["sums"].at[k, 1], (Z - 1) * q)
                res[here] = jnp.sum(top[...], axis=0)
                for dy, dx in spots[::-1]:
                    yy, xx = at(y, dy, Y), at(x, dx, X)
                    for cc in range(C):
                        if (dy, dx) != (0, 0) or cc != owner:
                            send(res.at[here], res.at[here], 2, dev(z, yy, xx, cc))

        def step3():
            pl.when(~owns)(lambda: arrive(r["sums"].at[k, 2], n * q))
            if n > 1:
                pl.when(owns)(lambda: arrive(r["sums"].at[k, 2], (n - 1) * q))

        def drain():
            pl.when(owns)(lambda: tally((n - 1 + Z - 1 + 2 * n - 1) * q, leaves).wait_send())
            if not per_chip:
                pl.when(~owns)(lambda: tally(n * q, leaves).wait_send())

        def total():
            return jnp.concatenate([res[w] for w in range(n)], axis=0)

        return [step0, step1, step2, step3], total, drain

    def head(name, count, *index):
        return r[name].at[(*index, pl.ds(0, count))]

    def rs1(h, s):
        for w in range(X * Y):
            part[h, s, w // X, w % X] = dot(gt[s, w], r["weights"][h, 0]) + dot(gt[s, w], r["weights"][h, 1])
        if s == 1 and keep is not None:
            for dy, dx in other_rows:
                copy(part.at[h, s, at(y, dy, Y), at(x, dx, X), middle], r["ebuf"].at[h, dy, dx],
                     r["rse"].at[h], dev(near(1), y, x, c))
        if s == 0 and keep is not None:
            arrive(r["rse"].at[h], len(other_rows) * middle.size)
            for dy, dx in other_rows:
                ref = part.at[h, s, at(y, dy, Y), at(x, dx, X), middle]
                ref[...] = ref[...] + r["ebuf"][h, dy, dx]
        for dy in dys:
            for dx in dxs:
                yy, xx = at(y, dy, Y), at(x, dx, X)
                copy(part.at[h, s, yy, xx, low(s)], head("rda", n_low(s), h, s, dy, dx), r["rsf"].at[h, s],
                     dev(z, yy, x, c))
                copy(part.at[h, s, yy, xx, high(s)], head("rdb", n_high(s), h, s, dy, dx), r["rsf"].at[h, s],
                     dev(z, y, xx, c))
        for dy in dys:
            yy = at(y, dy, Y)
            copy(part.at[h, s, yy, x, low(s)], head("rya", n_low(s), h, s, dy), r["rsr"].at[h, s], dev(z, yy, x, c))
        for dx in dxs:
            xx = at(x, dx, X)
            copy(part.at[h, s, y, xx, high(s)], head("rxb", n_high(s), h, s, dx), r["rsr"].at[h, s], dev(z, y, xx, c))

    def rs2(h, s):
        if dxs and dys:
            arrive(r["rsf"].at[h, s], len(dxs) * len(dys) * (n_low(s) + n_high(s)))
        for dx in dxs:
            xx = at(x, dx, X)
            ref = part.at[h, s, y, xx, low(s)]
            total = ref[...]
            for dy in dys:
                total = total + head("rda", n_low(s), h, s, dy, dx)[...]
            ref[...] = total
            copy(ref, head("rxa", n_low(s), h, s, dx), r["rsr"].at[h, s], dev(z, y, xx, c))
        for dy in dys:
            yy = at(y, dy, Y)
            ref = part.at[h, s, yy, x, high(s)]
            total = ref[...]
            for dx in dxs:
                total = total + head("rdb", n_high(s), h, s, dy, dx)[...]
            ref[...] = total
            copy(ref, head("ryb", n_high(s), h, s, dy), r["rsr"].at[h, s], dev(z, yy, x, c))

    fin = r["fin"]

    def rs3(h, s):
        if dxs or dys:
            arrive(r["rsr"].at[h, s], (len(dxs) + len(dys)) * (n_low(s) + n_high(s)))
        total = part[h, s, y, x, low(s)]
        for name, ds in (("rya", dys), ("rxa", dxs)):
            for d in ds:
                total = total + head(name, n_low(s), h, s, d)[...]
        fin[h, s, low(s)] = total
        total = part[h, s, y, x, high(s)]
        for name, ds in (("rxb", dxs), ("ryb", dys)):
            for d in ds:
                total = total + head(name, n_high(s), h, s, d)[...]
        fin[h, s, high(s)] = total
        if s == 1 and keep is not None:
            fin[h, s, middle] = part[h, s, y, x, middle]
        if s:
            copy(fin.at[h, s], r["rz"].at[h, z], r["rsz"].at[h], dev(near(s), y, x, c))

    def collect():
        got = []
        for h in range(G):
            total = fin[h, 0]
            if Z > 1:
                arrive(r["rsz"].at[h], (Z - 1) * deep)
            for p in range(1, Z):
                total = total + r["rz"][h, near(p)]
            got.append(total)
        if G == 1:
            r["raw"][...] = got[0]
        else:
            r["raw"][:deep] = jnp.where(lanes < wide, got[0], pltpu.roll(got[1], wide, 1))
            r["raw"][deep:] = jnp.where(lanes < wide, pltpu.roll(got[0], wide, 1), got[1])

    aug = r["aug"]
    lane = lax.broadcasted_iota(jnp.int32, (rank, rank), 1)
    row_of = lax.broadcasted_iota(jnp.int32, (rank, rank), 0)

    def eliminate(p, _):
        first = pl.multiple_of(p * PANEL, PANEL)
        lanes = lane[:PANEL]
        index = row_of[:PANEL, :1]
        block = aug[pl.ds(first, PANEL), :]
        left = block[:, :rank]
        cols = [
            jnp.sum(jnp.where(lanes == first + k, left, 0.0), axis=1, keepdims=True)
            for k in range(PANEL)
        ]
        scale = jnp.zeros((PANEL, 1), F32)
        for k in range(PANEL):
            inv = 1.0 / cols[k][k : k + 1]
            f = jnp.where(index > k, cols[k] * inv, 0.0)
            for m in range(k + 1, PANEL):
                cols[m] = cols[m] - f * cols[m][k : k + 1]
            block = block - f * block[k : k + 1]
            scale = jnp.where(index == k, inv, scale)
        u = thirds(jnp.where(lanes >= first + PANEL, block[:, :rank] * scale, 0.0))
        v = thirds(block)
        lhs = jnp.concatenate([u[i] for i in (0, 0, 0, 1, 1, 2)], axis=0).astype(BF16)
        rhs = jnp.concatenate([v[i] for i in (0, 1, 2, 0, 1, 0)], axis=0).astype(BF16)
        aug[...] = aug[...] - dot(lhs, rhs, ((0,), (0,)))
        aug[pl.ds(first, PANEL), :] = block
        return 0

    def begin():
        aug[:, :rank] = gram_total()
        aug[:, rank:] = jnp.where(lane == row_of, 1.0, 0.0)

    def chol(first, last):
        lax.fori_loop(first, last, eliminate, 0)

    def finish():
        diag = jnp.sum(jnp.where(lane == row_of, aug[:, :rank], 0.0), axis=1, keepdims=True)
        inverse = aug[:, rank:] * lax.rsqrt(diag)
        inverse_out[...] = inverse
        basis[...] = jnp.sqrt(F32(total_pixels)) * exact(r["sketched"][mine], inverse, ((1,), (1,)))
        projection[...] = exact(r["raw"][...], inverse, ((1,), (1,)))

    def gram_part():
        v = r["sketched"][...]
        return exact(v, v, ((0,), (0,)))

    def raw_part():
        v = r["raw"][...]
        return exact(v, v, ((0,), (0,)))

    gram, gram_total, drain_gram = total_sum(0, gram_part, True)
    spectrum, spectrum_total, drain_spectrum = total_sum(1, raw_part, False)
    panels = rank // PANEL

    def panel(i):
        if i == 0:
            begin()
        chol(panels * i // PARTS, panels * (i + 1) // PARTS)

    def send_own(h):
        in_plane(h, 0)
        if h == 0:
            swap()

    def give_take(h):
        take(h)
        if h == G - 1:
            merge()

    def prepare(s):
        if not prepared:
            swapped()
        prepared.add(s)
        prep(s)

    prepared = set()
    steps = dict(
        ownp=send_own, ownz=to_plane, prep=prepare, zin=zin, diag=diag, share=share, fin=multiply, give=give,
        take=give_take, rs1=rs1, rs2=rs2, rs3=rs3, collect=collect, sum=lambda k, i: (gram, spectrum)[k][i](),
        panel=panel, finish=finish,
    )
    for name, *index in schedule(G, Z):
        steps[name](*index)
    spec[...] = spectrum_total()
    finish_sends()


def finish_kernel(patches, basis_in, projection_in, inverse_in, spec_in, basis, projection, spectrum):
    inverse = inverse_in[...]
    basis[...] = basis_in[...]
    projection[...] = projection_in[...]
    spectrum[...] = exact(exact(inverse, spec_in[...]), inverse, ((1,), (1,))) / F32(patches)


def body(grid, green, sketch):
    C, X, Y, Z = grid
    rows, rank = sketch.shape
    pixels, patches = green.shape
    G, deep, half, keep = layout_of(grid, rows, rank)
    other = deep - half
    both = C * pixels
    few = rank // (X * Y)

    def vmem(*shape):
        return pltpu.VMEM(shape, F32)

    def packed(*shape):
        return pltpu.VMEM(shape, BF16)

    def dma(*shape):
        return pltpu.SemaphoreType.DMA(shape)

    flags = pltpu.SemaphoreType.REGULAR((Z,))
    links = X - 1 + Y - 1 + (X - 1) * (Y - 1)
    count = 2 * G * deep * ((Z + 1) * links + Z - 1) + G * both
    scratch = dict(
        green=vmem(both, patches), sketch=vmem(rows, rank), gat=vmem(G, Z, Y, X, deep, rank),
        turned=vmem(X * Y * C * rows, both),
        gl=packed(Z, X * Y, 2 * G * both, deep), gt=packed(Z, X * Y, deep, 2 * G * both),
        acc=vmem(G, G * both, rank), mine=vmem(G, both, rank), theirs=vmem(G, both, rank),
        folded=vmem(G, both, rank), weights=packed(G, 2, 2 * G * both, rank), sketched=vmem(both, rank),
        part=vmem(G, Z, Y, X, deep, rank),
        rda=vmem(G, Z, Y, X, half, rank), rdb=vmem(G, Z, Y, X, other, rank),
        rya=vmem(G, Z, Y, half, rank), rxb=vmem(G, Z, X, other, rank),
        rxa=vmem(G, Z, X, half, rank), ryb=vmem(G, Z, Y, other, rank),
        ebuf=vmem(G, Y, X, max(8, deep - 2 * (keep or 0)), rank),
        fin=vmem(G, Z, deep, rank), rz=vmem(G, Z, deep, rank), raw=vmem(rows, rank),
        t_src=vmem(2, X * Y, few, rank), t_in=vmem(2, C, X * Y, few, rank),
        t_top=vmem(2, Z, few, rank), t_res=vmem(2, X * Y, few, rank),
        aug=vmem(rank, 2 * rank), kup=flags, kdown=flags,
        tally=vmem(count, rank),
        send=dma(1), load=dma(2), swap=dma(1 + G), swap_send=dma(1),
        agz=dma(G, Z), agf=dma(G, Z), agr=dma(G, Z),
        rsf=dma(G, Z), rsr=dma(G, Z), rsz=dma(G), age=dma(G), rse=dma(G), sums=dma(2, 3), sums_send=dma(2),
    )
    total_pixels = pixels * C * X * Y * Z
    tall = jax.ShapeDtypeStruct((pixels, rank), F32)
    wide = jax.ShapeDtypeStruct((rows, rank), F32)
    square = jax.ShapeDtypeStruct((rank, rank), F32)
    whole = pl.BlockSpec(memory_space=pltpu.VMEM)
    parts = pl.pallas_call(
        functools.partial(kernel, grid, total_pixels),
        out_shape=(tall, wide, square, square),
        in_specs=[pl.BlockSpec(memory_space=pl.ANY)] * 2,
        out_specs=(whole,) * 4,
        scratch_shapes=[scratch],
        compiler_params=pltpu.CompilerParams(
            collective_id=0, has_side_effects=True, vmem_limit_bytes=int(VLIM * 2**20)
        ),
    )(green, sketch)
    return pl.pallas_call(
        functools.partial(finish_kernel, patches),
        out_shape=(tall, wide, square),
        in_specs=[whole] * 4,
        out_specs=(whole,) * 3,
        compiler_params=pltpu.CompilerParams(vmem_limit_bytes=2**20),
    )(*parts)


def solution(mesh):
    grid = grid_of(mesh.shape["pix"])
    in_specs = (P("pix", None), P("pix", None))
    out_specs = (P("pix", None), P("pix", None), P())
    return jax.shard_map(
        functools.partial(body, grid), mesh=mesh, in_specs=in_specs, out_specs=out_specs, check_vma=False
    )
```

```python
import functools
import math

import jax
import jax.numpy as jnp
from jax import lax
from jax.experimental import pallas as pl
from jax.experimental.pallas import tpu as pltpu
from jax.sharding import PartitionSpec as P

MESH = pl.DeviceIdType.MESH
F32 = jnp.float32
BF16 = jnp.bfloat16
PANEL = 8
PARTS = 8
PAIRED = True
VLIM = 53.63
KEEP = 6
SHARES = (0, 0)


def grid_of(devices):
    cores = 2 if devices % 2 == 0 else 1
    chips = devices // cores
    side = 1
    for k in range(1, chips + 1):
        if chips % (k * k) == 0 and k * k * k <= chips:
            side = k
    return cores, side, side, chips // (side * side)


def order_of(planes):
    table = []
    for z in range(planes):
        rest = sorted((k for k in range(planes) if k != z), key=lambda k: (abs(k - z), abs(2 * k - planes + 1)))
        if planes % 2 == 0 and PAIRED:
            rest.remove(z ^ 1)
            rest.insert(0, z ^ 1)
        table.append([z] + rest)
    return table


def layout_of(grid, rows, rank):
    C, X, Y, Z = grid
    parts = 2 if rows % 32 == 0 and rank == 128 else 1
    deep = rows // parts
    half = (deep // 2 + 7) // 8 * 8
    keep = min(max(8, KEEP * half // 6 // 8 * 8), deep - half)
    return parts, deep, half, keep if Z % 2 == 0 and X * Y > 1 and 0 < keep < half else None


PLANS = {
    (2, 4): [
        ("ownp", 0), ("ownz", 0, 1), ("ownp", 1), ("ownz", 0, 3), ("ownq", 1), ("ownq", 0), ("ownz", 0, 2),
        ("diag", 0, 0), ("zin", 0, 1), ("zot", 0, 1), ("prep", 3), ("ownz", 1, 1), ("diag", 1, 0),
        ("ownz", 1, 3), ("zin", 0, 2), ("ownz", 1, 2), ("zin", 0, 3), ("zot", 0, 2), ("zot", 0, 3),
        ("prep", 1), ("diag", 0, 1), ("zin", 1, 1), ("prep", 2), ("diag", 0, 2), ("prep", 0),
        ("diag", 0, 3), ("zin", 1, 2), ("zin", 1, 3), ("zot", 1, 1), ("zot", 1, 2), ("zot", 1, 3),
        ("fin", 0, 1), ("fin", 0, 0), ("diag", 1, 1), ("fin", 0, 2), ("fin", 0, 3), ("give", 0),
        ("diag", 1, 2), ("diag", 1, 3), ("take", 0), ("rs1", 0, 1), ("rs1", 0, 2), ("rst", 0, 2),
        ("rs1", 0, 3), ("fin", 1, 1), ("rst", 0, 1), ("fin", 1, 0), ("fin", 1, 2), ("rst", 0, 3),
        ("fin", 1, 3), ("give", 1), ("rs2", 0, 1), ("rs2", 0, 2), ("take", 1), ("rs1", 1, 3),
        ("sum", 0, 0), ("rs1", 1, 1), ("rs2", 0, 3), ("rs1", 1, 2), ("rs3", 0, 1), ("rs3", 0, 2),
        ("rst", 1, 3), ("rs2", 1, 3), ("rs1", 1, 0), ("sum", 0, 1), ("rst", 1, 2), ("rs2", 1, 1),
        ("rst", 1, 1), ("rs2", 1, 2), ("rs3", 0, 3), ("rs1", 0, 0), ("rst", 0, 0), ("rst", 1, 0),
        ("rs3", 1, 3), ("sum", 0, 2), ("rs3", 1, 1), ("rs2", 1, 0), ("rs3", 1, 2), ("rs2", 0, 0),
        ("sum", 0, 3), ("panel", 0), ("rs3", 1, 0), ("rs3", 0, 0), ("collect",), ("sum", 1, 0),
        ("panel", 1), ("panel", 2), ("panel", 3), ("sum", 1, 1), ("panel", 4), ("panel", 5), ("sum", 1, 2),
        ("panel", 6), ("panel", 7), ("finish",), ("sum", 1, 3),
    ],
}


def schedule(parts, planes):
    tuned = PLANS.get((parts, planes))
    if tuned:
        return tuned
    near = range(planes)
    far = near[::-1]
    plan = []
    for h in range(parts):
        plan += [("ownp", h), ("ownq", h)] + [("ownz", h, p) for p in near[1:]]
    for h in range(parts):
        for p in near:
            plan += [("zin", h, p), ("zot", h, p)] * (p > 0) + [("diag", h, p)]
    plan += [("prep", p) for p in near] + [("share", h) for h in range(parts)]
    for h in range(parts):
        plan += [("fin", h, p) for p in near] + [("give", h)]
    plan += [("take", h) for h in range(parts)] + [("sum", 0, 0)]
    for h in range(parts):
        for p in far:
            plan += [("rs1", h, p), ("rst", h, p), ("rs2", h, p), ("rs3", h, p)]
    plan += [("sum", 0, 1), ("sum", 0, 2), ("collect",), ("sum", 1, 0), ("sum", 0, 3)]
    plan += [("sum", 1, 1)] + [("panel", i) for i in range(PARTS)] + [("finish",)]
    return plan + [("sum", 1, 2), ("sum", 1, 3)]

def split(v):
    hi = v.astype(BF16)
    return hi, (v - hi.astype(F32)).astype(BF16)


def thirds(v):
    a = v.astype(BF16).astype(F32)
    b = (v - a).astype(BF16).astype(F32)
    return a, b, v - a - b


def dot(a, b, dims=((1,), (0,))):
    return lax.dot_general(a, b, (dims, ((), ())), preferred_element_type=F32)


def exact(a, b, dims=((1,), (0,))):
    return lax.dot_general(
        a, b, (dims, ((), ())), precision=lax.Precision.HIGHEST, preferred_element_type=F32
    )


def kernel(grid, total_pixels, green_in, sketch_in, basis, projection, inverse_out, spec, scratch):
    C, X, Y, Z = grid
    assert C == 2
    r = scratch
    me = lax.axis_index("pix")
    c = lax.rem(me, C)
    x = lax.rem(me // C, X)
    y = lax.rem(me // (C * X), Y)
    z = me // (C * X * Y)
    green, sketch, gat, part = r["green"], r["sketch"], r["gat"], r["part"]
    rows, rank = sketch.shape
    pixels = green_in.shape[0]
    both = C * pixels
    G, deep, half, keep = layout_of(grid, rows, rank)
    wide = rank // G
    slab = X * Y * C * rows
    table = order_of(Z)
    mine = pl.ds(pl.multiple_of(c * pixels, 8), pixels)
    rest = deep - half
    other_rows = [(dy, dx) for dy in range(Y) for dx in range(X) if (dy, dx) != (0, 0)]
    middle = pl.ds(keep or 0, deep - 2 * (keep or 0))

    keep_g, keep_s = (keep if on else None for on in SHARES)

    def low(s, keep):
        return pl.ds(0, half if keep is None or s != 1 else keep)

    def high(s, keep):
        return pl.ds(half, rest) if keep is None or s != 1 else pl.ds(deep - keep, keep)

    def n_low(s, keep):
        return low(s, keep).size

    def n_high(s, keep):
        return high(s, keep).size


    def dev(zz, yy, xx, cc):
        return (((zz * Y + yy) * X + xx) * C + cc,)

    def at(v, d, n):
        return lax.rem(v + d + n, n)

    def near(p):
        out = table[0][p]
        for k in range(1, Z):
            out = jnp.where(z == k, table[k][p], out)
        return out

    partner = dev(z, y, x, 1 - c)
    dxs, dys = range(1, X), range(1, Y)
    counter = [0]
    sends = []

    sent = [0]

    def copy(src, dst, recv, to, leaves=None):
        pltpu.make_async_remote_copy(
            src_ref=src, dst_ref=dst, send_sem=r["send"].at[0] if leaves is None else leaves, recv_sem=recv,
            device_id=to, device_id_type=MESH,
        ).start()
        if leaves is None:
            sent[0] += math.prod(src.shape) // rank

    def tally(count, leaves):
        ref = r["tally"].at[pl.ds(0, count)]
        return pltpu.make_async_remote_copy(
            src_ref=ref, dst_ref=ref, send_sem=leaves, recv_sem=leaves,
            device_id=partner, device_id_type=MESH,
        )

    def arrive(recv, count):
        ref = r["tally"].at[pl.ds(0, count)]
        pltpu.make_async_remote_copy(
            src_ref=ref, dst_ref=ref, send_sem=r["send"].at[0], recv_sem=recv,
            device_id=partner, device_id_type=MESH,
        ).wait_recv()

    def finish_sends():
        tally(sent[0], r["send"].at[0]).wait_send()
        drain_gram()
        drain_spectrum()

    load_sketch = pltpu.make_async_copy(sketch_in, sketch, r["load"].at[0])
    load_green = pltpu.make_async_copy(green_in, green.at[mine], r["load"].at[1])
    load_sketch.start()
    load_green.start()
    barrier = pltpu.get_barrier_semaphore()
    peers = [(partner, None)]
    peers += [(dev(z, y, at(x, dx, X), c), None) for dx in dxs]
    peers += [(dev(z, at(y, dy, Y), x, c), None) for dy in dys]
    peers += [(dev(z - 1, y, x, c), z > 0), (dev(z + 1, y, x, c), z < Z - 1)]

    def greet(peer):
        pl.semaphore_signal(barrier, inc=1, device_id=peer, device_id_type=MESH)

    for peer, when in peers:
        if when is None:
            greet(peer)
        else:
            pl.when(when)(functools.partial(greet, peer))
    lanes = lax.broadcasted_iota(jnp.int32, (deep, rank), 1)
    load_sketch.wait()
    if G == 1:
        gat[0, z, y, x] = sketch[...]
    else:
        top, bottom = sketch[:deep], sketch[deep:]
        gat[0, z, y, x] = jnp.where(lanes < wide, top, pltpu.roll(bottom, wide, 1))
        gat[1, z, y, x] = jnp.where(lanes < wide, pltpu.roll(top, wide, 1), bottom)
    known = len(peers) - 2 + jnp.where(z > 0, 1, 0) + jnp.where(z < Z - 1, 1, 0)
    pl.semaphore_wait(barrier, known)

    def along_x(h, s, k):
        ref = gat.at[h, near(s), y, x, (low, high)[k](s, keep_g)]
        for dx in dxs:
            copy(ref, ref, r["agr" if k else "agf"].at[h, s], dev(z, y, at(x, dx, X), c))

    def along_y(h, s, k):
        ref = gat.at[h, near(s), y, x, (low, high)[k](s, keep_g)]
        for dy in dys:
            copy(ref, ref, r["agf" if k else "agr"].at[h, s], dev(z, at(y, dy, Y), x, c))

    def in_plane(h, s):
        along_x(h, s, 0)
        along_y(h, s, 1)

    def in_plane_rest(h, s=0):
        along_x(h, s, 1)
        along_y(h, s, 0)

    def tell(sem, to):
        pl.semaphore_signal(sem, inc=1, device_id=to, device_id_type=MESH)

    def learn(j):
        up, down = r["kup"].at[j], r["kdown"].at[j]
        pl.when((z >= 1) & (z + j < Z))(functools.partial(tell, up, dev(z - 1, y, x, c)))
        pl.when((z + 1 < Z) & (z - j >= 0))(functools.partial(tell, down, dev(z + 1, y, x, c)))

    def known_far(j):
        pl.when(z + 1 + j < Z)(lambda: pl.semaphore_wait(r["kup"].at[j], 1))
        pl.when(z - 1 - j >= 0)(lambda: pl.semaphore_wait(r["kdown"].at[j], 1))

    reach = [0]

    def to_plane(h, p):
        far = max(abs(row[p] - row[0]) for row in table)
        while reach[0] < far - 1:
            reach[0] += 1
            learn(reach[0])
            known_far(reach[0])
        ref = gat.at[h, z, y, x]
        copy(ref, ref, r["agz"].at[h, z], dev(near(p), y, x, c))

    def zin(h, s):
        arrive(r["agz"].at[h, near(s)], deep)
        in_plane(h, s)

    def diag(h, s):
        zc = near(s)
        if dxs or dys:
            arrive(r["agf"].at[h, s], len(dxs) * n_low(s, keep_g) + len(dys) * n_high(s, keep_g))
        for dx in dxs:
            for dy in dys:
                ref = gat.at[h, zc, y, at(x, -dx, X), low(s, keep_g)]
                copy(ref, ref, r["agr"].at[h, s], dev(z, at(y, dy, Y), x, c))
        for dy in dys:
            for dx in dxs:
                ref = gat.at[h, zc, at(y, -dy, Y), x, high(s, keep_g)]
                copy(ref, ref, r["agr"].at[h, s], dev(z, y, at(x, dx, X), c))

    def swap():
        pltpu.make_async_remote_copy(
            src_ref=green_in, dst_ref=green.at[mine], send_sem=r["swap_send"].at[0], recv_sem=r["swap"].at[0],
            device_id=partner, device_id_type=MESH,
        ).start()

    def swapped():
        other = green.at[pl.ds(pl.multiple_of((1 - c) * pixels, 8), pixels)]
        load_green.wait()
        pltpu.make_async_remote_copy(
            src_ref=green_in, dst_ref=other, send_sem=r["swap_send"].at[0], recv_sem=r["swap"].at[0],
            device_id=partner, device_id_type=MESH,
        ).wait()

    gl, gt, turned = r["gl"], r["gt"], r["turned"]

    def prep(s):
        g = green[:, pl.ds(pl.multiple_of(near(s) * slab, 128), slab)]
        turned[...] = g.T
        for w in range(X * Y):
            block = turned[pl.ds(pl.multiple_of(w * C * rows + c * rows, 8), rows)]
            hi, lo = split(block)
            gt[s, w] = jnp.concatenate(
                [v[g * deep : (g + 1) * deep] for g in range(G) for v in (hi, lo)], axis=1
            )
            halves = [split(block[g * deep : (g + 1) * deep].T) for g in range(G)]
            gl[s, w] = jnp.concatenate([v[0] for v in halves] + [v[1] for v in halves], axis=0)

    started = set()

    gathered = set()

    def in_hand(h, s):
        if (dxs or dys) and (h, s) not in gathered:
            gathered.add((h, s))
            diags = len(dxs) * len(dys)
            count = (len(dxs) + diags) * n_high(s, keep_g) + (len(dys) + diags) * n_low(s, keep_g)
            arrive(r["agr"].at[h, s], count)

    def share(h):
        if keep_g is not None:
            in_hand(h, 0)
            for dy, dx in other_rows:
                ref = gat.at[h, z, at(y, dy, Y), at(x, dx, X), middle]
                copy(ref, ref, r["age"].at[h], dev(near(1), y, x, c))

    def multiply(h, s):
        in_hand(h, s)
        if s == 1 and keep_g is not None:
            arrive(r["age"].at[h], len(other_rows) * middle.size)
        zc = near(s)
        out = None
        for w in range(X * Y):
            b_hi, b_lo = split(gat[h, zc, w // X, w % X])
            tall = dot(gl[s, w], b_hi)
            term = tall[: G * both] + tall[G * both :] + dot(gl[s, w, : G * both], b_lo)
            out = term if out is None else out + term
        if h in started:
            r["acc"][h] += out
        else:
            started.add(h)
            r["acc"][h] = out

    lane_b = lax.broadcasted_iota(jnp.int32, (both, rank), 1)

    def give(h):
        v = r["acc"][h]
        if G == 2:
            v = jnp.where(lane_b < wide, v[:both], v[both:])
        r["mine"][h] = v
        copy(r["mine"].at[h], r["theirs"].at[h], r["swap"].at[1 + h], partner)

    weights = {}

    def take(h):
        arrive(r["swap"].at[1 + h], both)
        v = r["mine"][h] + r["theirs"][h]
        if G == 2:
            v = v + pltpu.roll(v, wide, 1)
        r["folded"][h] = v
        tall = [v] if G == 1 else [jnp.where(lane_b < wide, v, 0.0), jnp.where(lane_b < wide, 0.0, v)]
        pairs = [split(t) for t in tall]
        for i in range(2):
            r["weights"][h, i] = jnp.concatenate([p[i] for p in pairs for _ in range(2)], axis=0)

    def merge():
        if G == 1:
            r["sketched"][...] = r["folded"][0]
        else:
            r["sketched"][...] = jnp.where(lane_b < wide, r["folded"][0], r["folded"][1])

    owner = C - 1
    owns = c == owner
    here = y * X + x
    q = rank // (X * Y)
    spots = [(dy, dx) for dy in range(Y) for dx in range(X)]
    n = len(spots)

    def total_sum(k, value, per_chip):
        src, inc, top, res = (r[n].at[k] for n in ("t_src", "t_in", "t_top", "t_res"))
        leaves = r["sums_send"].at[k]

        def send(ref, dst, step, to):
            copy(ref, dst, r["sums"].at[k, step], to, leaves)

        def scatter(skip):
            for dy, dx in spots[skip:]:
                yy, xx = at(y, dy, Y), at(x, dx, X)
                send(src.at[yy * X + xx], inc.at[c, dy * X + dx], 0, dev(z, yy, xx, owner))

        def step0():
            def fill():
                v = value()
                for w in range(n):
                    src[w] = v[w * q : (w + 1) * q]

            if per_chip:
                @pl.when(owns)
                def _():
                    fill()
                    scatter(1)
            else:
                fill()
                pl.when(owns)(lambda: scatter(1))
                pl.when(~owns)(lambda: scatter(0))

        def step1():
            @pl.when(owns)
            def _():
                total = src[here]
                arrive(r["sums"].at[k, 0], (n - 1 if per_chip else 2 * n - 1) * q)
                for i in range(n):
                    if i:
                        total = total + inc[owner, i]
                    if not per_chip:
                        total = total + inc[0, i]
                top[z] = total
                for p in range(1, Z):
                    send(top.at[z], top.at[z], 1, dev(near(p), y, x, owner))

        def step2():
            @pl.when(owns)
            def _():
                if Z > 1:
                    arrive(r["sums"].at[k, 1], (Z - 1) * q)
                res[here] = jnp.sum(top[...], axis=0)
                for dy, dx in spots[::-1]:
                    yy, xx = at(y, dy, Y), at(x, dx, X)
                    for cc in range(C):
                        if (dy, dx) != (0, 0) or cc != owner:
                            send(res.at[here], res.at[here], 2, dev(z, yy, xx, cc))

        def step3():
            pl.when(~owns)(lambda: arrive(r["sums"].at[k, 2], n * q))
            if n > 1:
                pl.when(owns)(lambda: arrive(r["sums"].at[k, 2], (n - 1) * q))

        def drain():
            pl.when(owns)(lambda: tally((n - 1 + Z - 1 + 2 * n - 1) * q, leaves).wait_send())
            if not per_chip:
                pl.when(~owns)(lambda: tally(n * q, leaves).wait_send())

        def total():
            return jnp.concatenate([res[w] for w in range(n)], axis=0)

        return [step0, step1, step2, step3], total, drain

    def head(name, count, *index):
        return r[name].at[(*index, pl.ds(0, count))]

    def rs1(h, s):
        for w in range(X * Y):
            part[h, s, w // X, w % X] = dot(gt[s, w], r["weights"][h, 0]) + dot(gt[s, w], r["weights"][h, 1])
        if s == 1 and keep_s is not None:
            for dy, dx in other_rows:
                copy(part.at[h, s, at(y, dy, Y), at(x, dx, X), middle], r["ebuf"].at[h, dy, dx],
                     r["rse"].at[h], dev(near(1), y, x, c))
        if s == 0 and keep_s is not None:
            arrive(r["rse"].at[h], len(other_rows) * middle.size)
            for dy, dx in other_rows:
                ref = part.at[h, s, at(y, dy, Y), at(x, dx, X), middle]
                ref[...] = ref[...] + r["ebuf"][h, dy, dx]
        for dy in dys:
            for dx in dxs:
                yy, xx = at(y, dy, Y), at(x, dx, X)
                copy(part.at[h, s, yy, xx, low(s, keep_s)], head("rda", n_low(s, keep_s), h, s, dy, dx), r["rsf"].at[h, s],
                     dev(z, yy, x, c))
                copy(part.at[h, s, yy, xx, high(s, keep_s)], head("rdb", n_high(s, keep_s), h, s, dy, dx), r["rsf"].at[h, s],
                     dev(z, y, xx, c))

    def rs_rest(h, s):
        for dy in dys:
            yy = at(y, dy, Y)
            copy(part.at[h, s, yy, x, low(s, keep_s)], head("rya", n_low(s, keep_s), h, s, dy), r["rsr"].at[h, s], dev(z, yy, x, c))
        for dx in dxs:
            xx = at(x, dx, X)
            copy(part.at[h, s, y, xx, high(s, keep_s)], head("rxb", n_high(s, keep_s), h, s, dx), r["rsr"].at[h, s], dev(z, y, xx, c))

    def rs2(h, s):
        if dxs and dys:
            arrive(r["rsf"].at[h, s], len(dxs) * len(dys) * (n_low(s, keep_s) + n_high(s, keep_s)))
        for dx in dxs:
            xx = at(x, dx, X)
            ref = part.at[h, s, y, xx, low(s, keep_s)]
            total = ref[...]
            for dy in dys:
                total = total + head("rda", n_low(s, keep_s), h, s, dy, dx)[...]
            ref[...] = total
            copy(ref, head("rxa", n_low(s, keep_s), h, s, dx), r["rsr"].at[h, s], dev(z, y, xx, c))
        for dy in dys:
            yy = at(y, dy, Y)
            ref = part.at[h, s, yy, x, high(s, keep_s)]
            total = ref[...]
            for dx in dxs:
                total = total + head("rdb", n_high(s, keep_s), h, s, dy, dx)[...]
            ref[...] = total
            copy(ref, head("ryb", n_high(s, keep_s), h, s, dy), r["rsr"].at[h, s], dev(z, yy, x, c))

    fin = r["fin"]

    def rs3(h, s):
        if dxs or dys:
            arrive(r["rsr"].at[h, s], (len(dxs) + len(dys)) * (n_low(s, keep_s) + n_high(s, keep_s)))
        total = part[h, s, y, x, low(s, keep_s)]
        for name, ds in (("rya", dys), ("rxa", dxs)):
            for d in ds:
                total = total + head(name, n_low(s, keep_s), h, s, d)[...]
        fin[h, s, low(s, keep_s)] = total
        total = part[h, s, y, x, high(s, keep_s)]
        for name, ds in (("rxb", dxs), ("ryb", dys)):
            for d in ds:
                total = total + head(name, n_high(s, keep_s), h, s, d)[...]
        fin[h, s, high(s, keep_s)] = total
        if s == 1 and keep_s is not None:
            fin[h, s, middle] = part[h, s, y, x, middle]
        if s:
            copy(fin.at[h, s], r["rz"].at[h, z], r["rsz"].at[h], dev(near(s), y, x, c))

    def collect():
        got = []
        for h in range(G):
            total = fin[h, 0]
            if Z > 1:
                arrive(r["rsz"].at[h], (Z - 1) * deep)
            for p in range(1, Z):
                total = total + r["rz"][h, near(p)]
            got.append(total)
        if G == 1:
            r["raw"][...] = got[0]
        else:
            r["raw"][:deep] = jnp.where(lanes < wide, got[0], pltpu.roll(got[1], wide, 1))
            r["raw"][deep:] = jnp.where(lanes < wide, pltpu.roll(got[0], wide, 1), got[1])

    aug = r["aug"]
    lane = lax.broadcasted_iota(jnp.int32, (rank, rank), 1)
    row_of = lax.broadcasted_iota(jnp.int32, (rank, rank), 0)

    def eliminate(p, _):
        first = pl.multiple_of(p * PANEL, PANEL)
        lanes = lane[:PANEL]
        index = row_of[:PANEL, :1]
        block = aug[pl.ds(first, PANEL), :]
        left = block[:, :rank]
        cols = [
            jnp.sum(jnp.where(lanes == first + k, left, 0.0), axis=1, keepdims=True)
            for k in range(PANEL)
        ]
        scale = jnp.zeros((PANEL, 1), F32)
        for k in range(PANEL):
            inv = 1.0 / cols[k][k : k + 1]
            f = jnp.where(index > k, cols[k] * inv, 0.0)
            for m in range(k + 1, PANEL):
                cols[m] = cols[m] - f * cols[m][k : k + 1]
            block = block - f * block[k : k + 1]
            scale = jnp.where(index == k, inv, scale)
        u = thirds(jnp.where(lanes >= first + PANEL, block[:, :rank] * scale, 0.0))
        v = thirds(block)
        lhs = jnp.concatenate([u[i] for i in (0, 0, 0, 1, 1, 2)], axis=0).astype(BF16)
        rhs = jnp.concatenate([v[i] for i in (0, 1, 2, 0, 1, 0)], axis=0).astype(BF16)
        aug[...] = aug[...] - dot(lhs, rhs, ((0,), (0,)))
        aug[pl.ds(first, PANEL), :] = block
        return 0

    def begin():
        aug[:, :rank] = gram_total()
        aug[:, rank:] = jnp.where(lane == row_of, 1.0, 0.0)

    def chol(first, last):
        lax.fori_loop(first, last, eliminate, 0)

    def finish():
        diag = jnp.sum(jnp.where(lane == row_of, aug[:, :rank], 0.0), axis=1, keepdims=True)
        inverse = aug[:, rank:] * lax.rsqrt(diag)
        inverse_out[...] = inverse
        basis[...] = jnp.sqrt(F32(total_pixels)) * exact(r["sketched"][mine], inverse, ((1,), (1,)))
        projection[...] = exact(r["raw"][...], inverse, ((1,), (1,)))

    def gram_part():
        v = r["sketched"][...]
        return exact(v, v, ((0,), (0,)))

    def raw_part():
        v = r["raw"][...]
        return exact(v, v, ((0,), (0,)))

    gram, gram_total, drain_gram = total_sum(0, gram_part, True)
    spectrum, spectrum_total, drain_spectrum = total_sum(1, raw_part, False)
    panels = rank // PANEL

    def panel(i):
        if i == 0:
            begin()
        chol(panels * i // PARTS, panels * (i + 1) // PARTS)

    def send_own(h):
        in_plane(h, 0)
        if h == 0:
            swap()

    def give_take(h):
        take(h)
        if h == G - 1:
            merge()

    def prepare(s):
        if not prepared:
            swapped()
        prepared.add(s)
        prep(s)

    prepared = set()
    steps = dict(
        ownp=send_own, ownz=to_plane, prep=prepare, zin=zin, ownq=in_plane_rest, zot=in_plane_rest, rst=rs_rest, diag=diag, share=share, fin=multiply, give=give,
        take=give_take, rs1=rs1, rs2=rs2, rs3=rs3, collect=collect, sum=lambda k, i: (gram, spectrum)[k][i](),
        panel=panel, finish=finish,
    )
    for name, *index in schedule(G, Z):
        steps[name](*index)
    spec[...] = spectrum_total()
    finish_sends()


def finish_kernel(patches, basis_in, projection_in, inverse_in, spec_in, basis, projection, spectrum):
    inverse = inverse_in[...]
    basis[...] = basis_in[...]
    projection[...] = projection_in[...]
    spectrum[...] = exact(exact(inverse, spec_in[...]), inverse, ((1,), (1,))) / F32(patches)


def body(grid, green, sketch):
    C, X, Y, Z = grid
    rows, rank = sketch.shape
    pixels, patches = green.shape
    G, deep, half, keep = layout_of(grid, rows, rank)
    other = deep - half
    both = C * pixels
    few = rank // (X * Y)

    def vmem(*shape):
        return pltpu.VMEM(shape, F32)

    def packed(*shape):
        return pltpu.VMEM(shape, BF16)

    def dma(*shape):
        return pltpu.SemaphoreType.DMA(shape)

    flags = pltpu.SemaphoreType.REGULAR((Z,))
    links = X - 1 + Y - 1 + (X - 1) * (Y - 1)
    count = 2 * G * deep * ((Z + 1) * links + Z - 1) + G * both
    scratch = dict(
        green=vmem(both, patches), sketch=vmem(rows, rank), gat=vmem(G, Z, Y, X, deep, rank),
        turned=vmem(X * Y * C * rows, both),
        gl=packed(Z, X * Y, 2 * G * both, deep), gt=packed(Z, X * Y, deep, 2 * G * both),
        acc=vmem(G, G * both, rank), mine=vmem(G, both, rank), theirs=vmem(G, both, rank),
        folded=vmem(G, both, rank), weights=packed(G, 2, 2 * G * both, rank), sketched=vmem(both, rank),
        part=vmem(G, Z, Y, X, deep, rank),
        rda=vmem(G, Z, Y, X, half, rank), rdb=vmem(G, Z, Y, X, other, rank),
        rya=vmem(G, Z, Y, half, rank), rxb=vmem(G, Z, X, other, rank),
        rxa=vmem(G, Z, X, half, rank), ryb=vmem(G, Z, Y, other, rank),
        ebuf=vmem(G, Y, X, max(8, deep - 2 * (keep or 0)), rank),
        fin=vmem(G, Z, deep, rank), rz=vmem(G, Z, deep, rank), raw=vmem(rows, rank),
        t_src=vmem(2, X * Y, few, rank), t_in=vmem(2, C, X * Y, few, rank),
        t_top=vmem(2, Z, few, rank), t_res=vmem(2, X * Y, few, rank),
        aug=vmem(rank, 2 * rank), kup=flags, kdown=flags,
        tally=vmem(count, rank),
        send=dma(1), load=dma(2), swap=dma(1 + G), swap_send=dma(1),
        agz=dma(G, Z), agf=dma(G, Z), agr=dma(G, Z),
        rsf=dma(G, Z), rsr=dma(G, Z), rsz=dma(G), age=dma(G), rse=dma(G), sums=dma(2, 3), sums_send=dma(2),
    )
    total_pixels = pixels * C * X * Y * Z
    tall = jax.ShapeDtypeStruct((pixels, rank), F32)
    wide = jax.ShapeDtypeStruct((rows, rank), F32)
    square = jax.ShapeDtypeStruct((rank, rank), F32)
    whole = pl.BlockSpec(memory_space=pltpu.VMEM)
    parts = pl.pallas_call(
        functools.partial(kernel, grid, total_pixels),
        out_shape=(tall, wide, square, square),
        in_specs=[pl.BlockSpec(memory_space=pl.ANY)] * 2,
        out_specs=(whole,) * 4,
        scratch_shapes=[scratch],
        compiler_params=pltpu.CompilerParams(
            collective_id=0, has_side_effects=True, vmem_limit_bytes=int(VLIM * 2**20)
        ),
    )(green, sketch)
    return pl.pallas_call(
        functools.partial(finish_kernel, patches),
        out_shape=(tall, wide, square),
        in_specs=[whole] * 4,
        out_specs=(whole,) * 3,
        compiler_params=pltpu.CompilerParams(vmem_limit_bytes=2**20),
    )(*parts)


def solution(mesh):
    grid = grid_of(mesh.shape["pix"])
    in_specs = (P("pix", None), P("pix", None))
    out_specs = (P("pix", None), P("pix", None), P())
    return jax.shard_map(
        functools.partial(body, grid), mesh=mesh, in_specs=in_specs, out_specs=out_specs, check_vma=False
    )
```

```python
import functools
import math

import jax
import jax.numpy as jnp
from jax import lax
from jax.experimental import pallas as pl
from jax.experimental.pallas import tpu as pltpu
from jax.sharding import PartitionSpec as P

MESH = pl.DeviceIdType.MESH
F32 = jnp.float32
BF16 = jnp.bfloat16
PANEL = 8
PARTS = 8
PAIRED = True
VLIM = 53.63
KEEP = 6
SHARES = (0, 0)


def grid_of(devices):
    cores = 2 if devices % 2 == 0 else 1
    chips = devices // cores
    side = 1
    for k in range(1, chips + 1):
        if chips % (k * k) == 0 and k * k * k <= chips:
            side = k
    return cores, side, side, chips // (side * side)


def order_of(planes):
    table = []
    for z in range(planes):
        rest = sorted((k for k in range(planes) if k != z), key=lambda k: (abs(k - z), abs(2 * k - planes + 1)))
        if planes % 2 == 0 and PAIRED:
            rest.remove(z ^ 1)
            rest.insert(0, z ^ 1)
        table.append([z] + rest)
    return table


def layout_of(grid, rows, rank):
    C, X, Y, Z = grid
    parts = 2 if rows % 32 == 0 and rank == 128 else 1
    deep = rows // parts
    half = (deep // 2 + 7) // 8 * 8
    keep = min(max(8, KEEP * half // 6 // 8 * 8), deep - half)
    return parts, deep, half, keep if Z % 2 == 0 and X * Y > 1 and 0 < keep < half else None


PLANS = {
    (2, 4): [
        ("ownp", 0), ("ownz", 0, 1), ("ownp", 1), ("ownz", 0, 3), ("ownq", 1), ("ownq", 0), ("ownz", 0, 2),
        ("diag", 0, 0), ("zin", 0, 1), ("zot", 0, 1), ("prep", 3), ("ownz", 1, 1), ("diag", 1, 0),
        ("ownz", 1, 3), ("zin", 0, 2), ("ownz", 1, 2), ("zin", 0, 3), ("zot", 0, 2), ("zot", 0, 3),
        ("prep", 1), ("diag", 0, 1), ("zin", 1, 1), ("prep", 2), ("diag", 0, 2), ("prep", 0),
        ("diag", 0, 3), ("zin", 1, 2), ("zin", 1, 3), ("zot", 1, 1), ("zot", 1, 2), ("zot", 1, 3),
        ("fin", 0, 1), ("fin", 0, 0), ("fin", 0, 2), ("diag", 1, 1), ("fin", 0, 3), ("give", 0),
        ("diag", 1, 2), ("diag", 1, 3), ("take", 0), ("rs1", 0, 1), ("rs1", 0, 2), ("rst", 0, 2),
        ("rs1", 0, 3), ("fin", 1, 1), ("rst", 0, 1), ("fin", 1, 0), ("fin", 1, 2), ("rst", 0, 3),
        ("fin", 1, 3), ("give", 1), ("rs2", 0, 1), ("rs2", 0, 2), ("take", 1), ("rs1", 1, 3),
        ("sum", 0, 0), ("rs1", 1, 1), ("rs2", 0, 3), ("rs1", 1, 2), ("rs3", 0, 1), ("rs3", 0, 2),
        ("rst", 1, 3), ("rs2", 1, 3), ("rs1", 1, 0), ("sum", 0, 1), ("rst", 1, 2), ("rs2", 1, 1),
        ("rst", 1, 1), ("rs2", 1, 2), ("rs3", 0, 3), ("rs1", 0, 0), ("rst", 0, 0), ("rst", 1, 0),
        ("rs3", 1, 3), ("sum", 0, 2), ("rs3", 1, 1), ("rs2", 1, 0), ("rs3", 1, 2), ("rs2", 0, 0),
        ("sum", 0, 3), ("panel", 0), ("rs3", 1, 0), ("rs3", 0, 0), ("collect",), ("sum", 1, 0),
        ("panel", 1), ("panel", 2), ("panel", 3), ("sum", 1, 1), ("panel", 4), ("panel", 5), ("sum", 1, 2),
        ("panel", 6), ("panel", 7), ("finish",), ("sum", 1, 3),
    ],
}


def schedule(parts, planes):
    tuned = PLANS.get((parts, planes))
    if tuned:
        return tuned
    near = range(planes)
    far = near[::-1]
    plan = []
    for h in range(parts):
        plan += [("ownp", h), ("ownq", h)] + [("ownz", h, p) for p in near[1:]]
    for h in range(parts):
        for p in near:
            plan += [("zin", h, p), ("zot", h, p)] * (p > 0) + [("diag", h, p)]
    plan += [("prep", p) for p in near] + [("share", h) for h in range(parts)]
    for h in range(parts):
        plan += [("fin", h, p) for p in near] + [("give", h)]
    plan += [("take", h) for h in range(parts)] + [("sum", 0, 0)]
    for h in range(parts):
        for p in far:
            plan += [("rs1", h, p), ("rst", h, p), ("rs2", h, p), ("rs3", h, p)]
    plan += [("sum", 0, 1), ("sum", 0, 2), ("collect",), ("sum", 1, 0), ("sum", 0, 3)]
    plan += [("sum", 1, 1)] + [("panel", i) for i in range(PARTS)] + [("finish",)]
    return plan + [("sum", 1, 2), ("sum", 1, 3)]

def split(v):
    hi = v.astype(BF16)
    return hi, (v - hi.astype(F32)).astype(BF16)


def thirds(v):
    a = v.astype(BF16).astype(F32)
    b = (v - a).astype(BF16).astype(F32)
    return a, b, v - a - b


def dot(a, b, dims=((1,), (0,))):
    return lax.dot_general(a, b, (dims, ((), ())), preferred_element_type=F32)


def exact(a, b, dims=((1,), (0,))):
    return lax.dot_general(
        a, b, (dims, ((), ())), precision=lax.Precision.HIGHEST, preferred_element_type=F32
    )


def kernel(grid, total_pixels, green_in, sketch_in, basis, projection, inverse_out, spec, scratch):
    C, X, Y, Z = grid
    assert C == 2
    r = scratch
    me = lax.axis_index("pix")
    c = lax.rem(me, C)
    x = lax.rem(me // C, X)
    y = lax.rem(me // (C * X), Y)
    z = me // (C * X * Y)
    green, sketch, gat, part = r["green"], r["sketch"], r["gat"], r["part"]
    rows, rank = sketch.shape
    pixels = green_in.shape[0]
    both = C * pixels
    G, deep, half, keep = layout_of(grid, rows, rank)
    wide = rank // G
    slab = X * Y * C * rows
    table = order_of(Z)
    mine = pl.ds(pl.multiple_of(c * pixels, 8), pixels)
    rest = deep - half
    other_rows = [(dy, dx) for dy in range(Y) for dx in range(X) if (dy, dx) != (0, 0)]
    middle = pl.ds(keep or 0, deep - 2 * (keep or 0))

    keep_g, keep_s = (keep if on else None for on in SHARES)

    def low(s, keep):
        return pl.ds(0, half if keep is None or s != 1 else keep)

    def high(s, keep):
        return pl.ds(half, rest) if keep is None or s != 1 else pl.ds(deep - keep, keep)

    def n_low(s, keep):
        return low(s, keep).size

    def n_high(s, keep):
        return high(s, keep).size


    def dev(zz, yy, xx, cc):
        return (((zz * Y + yy) * X + xx) * C + cc,)

    def at(v, d, n):
        return lax.rem(v + d + n, n)

    def near(p):
        out = table[0][p]
        for k in range(1, Z):
            out = jnp.where(z == k, table[k][p], out)
        return out

    partner = dev(z, y, x, 1 - c)
    dxs, dys = range(1, X), range(1, Y)
    counter = [0]
    sends = []

    sent = [0]

    def copy(src, dst, recv, to, leaves=None):
        pltpu.make_async_remote_copy(
            src_ref=src, dst_ref=dst, send_sem=r["send"].at[0] if leaves is None else leaves, recv_sem=recv,
            device_id=to, device_id_type=MESH,
        ).start()
        if leaves is None:
            sent[0] += math.prod(src.shape) // rank

    def tally(count, leaves):
        ref = r["tally"].at[pl.ds(0, count)]
        return pltpu.make_async_remote_copy(
            src_ref=ref, dst_ref=ref, send_sem=leaves, recv_sem=leaves,
            device_id=partner, device_id_type=MESH,
        )

    def arrive(recv, count):
        ref = r["tally"].at[pl.ds(0, count)]
        pltpu.make_async_remote_copy(
            src_ref=ref, dst_ref=ref, send_sem=r["send"].at[0], recv_sem=recv,
            device_id=partner, device_id_type=MESH,
        ).wait_recv()

    def finish_sends():
        tally(sent[0], r["send"].at[0]).wait_send()
        drain_gram()
        drain_spectrum()

    load_sketch = pltpu.make_async_copy(sketch_in, sketch, r["load"].at[0])
    load_green = pltpu.make_async_copy(green_in, green.at[mine], r["load"].at[1])
    load_sketch.start()
    load_green.start()
    barrier = pltpu.get_barrier_semaphore()
    peers = [(partner, None)]
    peers += [(dev(z, y, at(x, dx, X), c), None) for dx in dxs]
    peers += [(dev(z, at(y, dy, Y), x, c), None) for dy in dys]
    peers += [(dev(z - 1, y, x, c), z > 0), (dev(z + 1, y, x, c), z < Z - 1)]

    def greet(peer):
        pl.semaphore_signal(barrier, inc=1, device_id=peer, device_id_type=MESH)

    for peer, when in peers:
        if when is None:
            greet(peer)
        else:
            pl.when(when)(functools.partial(greet, peer))
    lanes = lax.broadcasted_iota(jnp.int32, (deep, rank), 1)
    load_sketch.wait()
    if G == 1:
        gat[0, z, y, x] = sketch[...]
    else:
        top, bottom = sketch[:deep], sketch[deep:]
        gat[0, z, y, x] = jnp.where(lanes < wide, top, pltpu.roll(bottom, wide, 1))
        gat[1, z, y, x] = jnp.where(lanes < wide, pltpu.roll(top, wide, 1), bottom)
    known = len(peers) - 2 + jnp.where(z > 0, 1, 0) + jnp.where(z < Z - 1, 1, 0)
    pl.semaphore_wait(barrier, known)

    def along_x(h, s, k):
        ref = gat.at[h, near(s), y, x, (low, high)[k](s, keep_g)]
        for dx in dxs:
            copy(ref, ref, r["agr" if k else "agf"].at[h, s], dev(z, y, at(x, dx, X), c))

    def along_y(h, s, k):
        ref = gat.at[h, near(s), y, x, (low, high)[k](s, keep_g)]
        for dy in dys:
            copy(ref, ref, r["agf" if k else "agr"].at[h, s], dev(z, at(y, dy, Y), x, c))

    def in_plane(h, s):
        along_x(h, s, 0)
        along_y(h, s, 1)

    def in_plane_rest(h, s=0):
        along_x(h, s, 1)
        along_y(h, s, 0)

    def tell(sem, to):
        pl.semaphore_signal(sem, inc=1, device_id=to, device_id_type=MESH)

    def learn(j):
        up, down = r["kup"].at[j], r["kdown"].at[j]
        pl.when((z >= 1) & (z + j < Z))(functools.partial(tell, up, dev(z - 1, y, x, c)))
        pl.when((z + 1 < Z) & (z - j >= 0))(functools.partial(tell, down, dev(z + 1, y, x, c)))

    def known_far(j):
        pl.when(z + 1 + j < Z)(lambda: pl.semaphore_wait(r["kup"].at[j], 1))
        pl.when(z - 1 - j >= 0)(lambda: pl.semaphore_wait(r["kdown"].at[j], 1))

    reach = [0]

    def to_plane(h, p):
        far = max(abs(row[p] - row[0]) for row in table)
        while reach[0] < far - 1:
            reach[0] += 1
            learn(reach[0])
            known_far(reach[0])
        ref = gat.at[h, z, y, x]
        copy(ref, ref, r["agz"].at[h, z], dev(near(p), y, x, c))

    def zin(h, s):
        arrive(r["agz"].at[h, near(s)], deep)
        in_plane(h, s)

    def diag(h, s):
        zc = near(s)
        if dxs or dys:
            arrive(r["agf"].at[h, s], len(dxs) * n_low(s, keep_g) + len(dys) * n_high(s, keep_g))
        for dx in dxs:
            for dy in dys:
                ref = gat.at[h, zc, y, at(x, -dx, X), low(s, keep_g)]
                copy(ref, ref, r["agr"].at[h, s], dev(z, at(y, dy, Y), x, c))
        for dy in dys:
            for dx in dxs:
                ref = gat.at[h, zc, at(y, -dy, Y), x, high(s, keep_g)]
                copy(ref, ref, r["agr"].at[h, s], dev(z, y, at(x, dx, X), c))

    def swap():
        pltpu.make_async_remote_copy(
            src_ref=green_in, dst_ref=green.at[mine], send_sem=r["swap_send"].at[0], recv_sem=r["swap"].at[0],
            device_id=partner, device_id_type=MESH,
        ).start()

    def swapped():
        other = green.at[pl.ds(pl.multiple_of((1 - c) * pixels, 8), pixels)]
        load_green.wait()
        pltpu.make_async_remote_copy(
            src_ref=green_in, dst_ref=other, send_sem=r["swap_send"].at[0], recv_sem=r["swap"].at[0],
            device_id=partner, device_id_type=MESH,
        ).wait()

    gl, gt, turned = r["gl"], r["gt"], r["turned"]

    def prep(s):
        g = green[:, pl.ds(pl.multiple_of(near(s) * slab, 128), slab)]
        turned[...] = g.T
        for w in range(X * Y):
            block = turned[pl.ds(pl.multiple_of(w * C * rows + c * rows, 8), rows)]
            hi, lo = split(block)
            gt[s, w] = jnp.concatenate(
                [v[g * deep : (g + 1) * deep] for g in range(G) for v in (hi, lo)], axis=1
            )
            halves = [split(block[g * deep : (g + 1) * deep].T) for g in range(G)]
            gl[s, w] = jnp.concatenate([v[0] for v in halves] + [v[1] for v in halves], axis=0)

    started = set()

    gathered = set()

    def in_hand(h, s):
        if (dxs or dys) and (h, s) not in gathered:
            gathered.add((h, s))
            diags = len(dxs) * len(dys)
            count = (len(dxs) + diags) * n_high(s, keep_g) + (len(dys) + diags) * n_low(s, keep_g)
            arrive(r["agr"].at[h, s], count)

    def share(h):
        if keep_g is not None:
            in_hand(h, 0)
            for dy, dx in other_rows:
                ref = gat.at[h, z, at(y, dy, Y), at(x, dx, X), middle]
                copy(ref, ref, r["age"].at[h], dev(near(1), y, x, c))

    def multiply(h, s):
        in_hand(h, s)
        if s == 1 and keep_g is not None:
            arrive(r["age"].at[h], len(other_rows) * middle.size)
        zc = near(s)
        out = None
        for w in range(X * Y):
            b_hi, b_lo = split(gat[h, zc, w // X, w % X])
            tall = dot(gl[s, w], b_hi)
            term = tall[: G * both] + tall[G * both :] + dot(gl[s, w, : G * both], b_lo)
            out = term if out is None else out + term
        if h in started:
            r["acc"][h] += out
        else:
            started.add(h)
            r["acc"][h] = out

    lane_b = lax.broadcasted_iota(jnp.int32, (both, rank), 1)

    def give(h):
        v = r["acc"][h]
        if G == 2:
            v = jnp.where(lane_b < wide, v[:both], v[both:])
        r["mine"][h] = v
        copy(r["mine"].at[h], r["theirs"].at[h], r["swap"].at[1 + h], partner)

    weights = {}

    def take(h):
        arrive(r["swap"].at[1 + h], both)
        v = r["mine"][h] + r["theirs"][h]
        if G == 2:
            v = v + pltpu.roll(v, wide, 1)
        r["folded"][h] = v
        tall = [v] if G == 1 else [jnp.where(lane_b < wide, v, 0.0), jnp.where(lane_b < wide, 0.0, v)]
        pairs = [split(t) for t in tall]
        for i in range(2):
            r["weights"][h, i] = jnp.concatenate([p[i] for p in pairs for _ in range(2)], axis=0)

    def merge():
        if G == 1:
            r["sketched"][...] = r["folded"][0]
        else:
            r["sketched"][...] = jnp.where(lane_b < wide, r["folded"][0], r["folded"][1])

    owner = C - 1
    owns = c == owner
    here = y * X + x
    q = rank // (X * Y)
    spots = [(dy, dx) for dy in range(Y) for dx in range(X)]
    n = len(spots)

    def total_sum(k, value, per_chip):
        src, inc, top, res = (r[n].at[k] for n in ("t_src", "t_in", "t_top", "t_res"))
        leaves = r["sums_send"].at[k]

        def send(ref, dst, step, to):
            copy(ref, dst, r["sums"].at[k, step], to, leaves)

        def scatter(skip):
            for dy, dx in spots[skip:]:
                yy, xx = at(y, dy, Y), at(x, dx, X)
                send(src.at[yy * X + xx], inc.at[c, dy * X + dx], 0, dev(z, yy, xx, owner))

        def step0():
            def fill():
                v = value()
                for w in range(n):
                    src[w] = v[w * q : (w + 1) * q]

            if per_chip:
                @pl.when(owns)
                def _():
                    fill()
                    scatter(1)
            else:
                fill()
                pl.when(owns)(lambda: scatter(1))
                pl.when(~owns)(lambda: scatter(0))

        def step1():
            @pl.when(owns)
            def _():
                total = src[here]
                arrive(r["sums"].at[k, 0], (n - 1 if per_chip else 2 * n - 1) * q)
                for i in range(n):
                    if i:
                        total = total + inc[owner, i]
                    if not per_chip:
                        total = total + inc[0, i]
                top[z] = total
                for p in range(1, Z):
                    send(top.at[z], top.at[z], 1, dev(near(p), y, x, owner))

        def step2():
            @pl.when(owns)
            def _():
                if Z > 1:
                    arrive(r["sums"].at[k, 1], (Z - 1) * q)
                res[here] = jnp.sum(top[...], axis=0)
                for dy, dx in spots[::-1]:
                    yy, xx = at(y, dy, Y), at(x, dx, X)
                    for cc in range(C):
                        if (dy, dx) != (0, 0) or cc != owner:
                            send(res.at[here], res.at[here], 2, dev(z, yy, xx, cc))

        def step3():
            pl.when(~owns)(lambda: arrive(r["sums"].at[k, 2], n * q))
            if n > 1:
                pl.when(owns)(lambda: arrive(r["sums"].at[k, 2], (n - 1) * q))

        def drain():
            pl.when(owns)(lambda: tally((n - 1 + Z - 1 + 2 * n - 1) * q, leaves).wait_send())
            if not per_chip:
                pl.when(~owns)(lambda: tally(n * q, leaves).wait_send())

        def total():
            return jnp.concatenate([res[w] for w in range(n)], axis=0)

        return [step0, step1, step2, step3], total, drain

    def head(name, count, *index):
        return r[name].at[(*index, pl.ds(0, count))]

    def rs1(h, s):
        for w in range(X * Y):
            part[h, s, w // X, w % X] = dot(gt[s, w], r["weights"][h, 0]) + dot(gt[s, w], r["weights"][h, 1])
        if s == 1 and keep_s is not None:
            for dy, dx in other_rows:
                copy(part.at[h, s, at(y, dy, Y), at(x, dx, X), middle], r["ebuf"].at[h, dy, dx],
                     r["rse"].at[h], dev(near(1), y, x, c))
        if s == 0 and keep_s is not None:
            arrive(r["rse"].at[h], len(other_rows) * middle.size)
            for dy, dx in other_rows:
                ref = part.at[h, s, at(y, dy, Y), at(x, dx, X), middle]
                ref[...] = ref[...] + r["ebuf"][h, dy, dx]
        for dy in dys:
            for dx in dxs:
                yy, xx = at(y, dy, Y), at(x, dx, X)
                copy(part.at[h, s, yy, xx, low(s, keep_s)], head("rda", n_low(s, keep_s), h, s, dy, dx), r["rsf"].at[h, s],
                     dev(z, yy, x, c))
                copy(part.at[h, s, yy, xx, high(s, keep_s)], head("rdb", n_high(s, keep_s), h, s, dy, dx), r["rsf"].at[h, s],
                     dev(z, y, xx, c))

    def rs_rest(h, s):
        for dy in dys:
            yy = at(y, dy, Y)
            copy(part.at[h, s, yy, x, low(s, keep_s)], head("rya", n_low(s, keep_s), h, s, dy), r["rsr"].at[h, s], dev(z, yy, x, c))
        for dx in dxs:
            xx = at(x, dx, X)
            copy(part.at[h, s, y, xx, high(s, keep_s)], head("rxb", n_high(s, keep_s), h, s, dx), r["rsr"].at[h, s], dev(z, y, xx, c))

    def rs2(h, s):
        if dxs and dys:
            arrive(r["rsf"].at[h, s], len(dxs) * len(dys) * (n_low(s, keep_s) + n_high(s, keep_s)))
        for dx in dxs:
            xx = at(x, dx, X)
            ref = part.at[h, s, y, xx, low(s, keep_s)]
            total = ref[...]
            for dy in dys:
                total = total + head("rda", n_low(s, keep_s), h, s, dy, dx)[...]
            ref[...] = total
            copy(ref, head("rxa", n_low(s, keep_s), h, s, dx), r["rsr"].at[h, s], dev(z, y, xx, c))
        for dy in dys:
            yy = at(y, dy, Y)
            ref = part.at[h, s, yy, x, high(s, keep_s)]
            total = ref[...]
            for dx in dxs:
                total = total + head("rdb", n_high(s, keep_s), h, s, dy, dx)[...]
            ref[...] = total
            copy(ref, head("ryb", n_high(s, keep_s), h, s, dy), r["rsr"].at[h, s], dev(z, yy, x, c))

    fin = r["fin"]

    def rs3(h, s):
        if dxs or dys:
            arrive(r["rsr"].at[h, s], (len(dxs) + len(dys)) * (n_low(s, keep_s) + n_high(s, keep_s)))
        total = part[h, s, y, x, low(s, keep_s)]
        for name, ds in (("rya", dys), ("rxa", dxs)):
            for d in ds:
                total = total + head(name, n_low(s, keep_s), h, s, d)[...]
        fin[h, s, low(s, keep_s)] = total
        total = part[h, s, y, x, high(s, keep_s)]
        for name, ds in (("rxb", dxs), ("ryb", dys)):
            for d in ds:
                total = total + head(name, n_high(s, keep_s), h, s, d)[...]
        fin[h, s, high(s, keep_s)] = total
        if s == 1 and keep_s is not None:
            fin[h, s, middle] = part[h, s, y, x, middle]
        if s:
            copy(fin.at[h, s], r["rz"].at[h, z], r["rsz"].at[h], dev(near(s), y, x, c))

    def collect():
        got = []
        for h in range(G):
            total = fin[h, 0]
            if Z > 1:
                arrive(r["rsz"].at[h], (Z - 1) * deep)
            for p in range(1, Z):
                total = total + r["rz"][h, near(p)]
            got.append(total)
        if G == 1:
            r["raw"][...] = got[0]
        else:
            r["raw"][:deep] = jnp.where(lanes < wide, got[0], pltpu.roll(got[1], wide, 1))
            r["raw"][deep:] = jnp.where(lanes < wide, pltpu.roll(got[0], wide, 1), got[1])

    aug = r["aug"]
    lane = lax.broadcasted_iota(jnp.int32, (rank, rank), 1)
    row_of = lax.broadcasted_iota(jnp.int32, (rank, rank), 0)

    def eliminate(p, _):
        first = pl.multiple_of(p * PANEL, PANEL)
        lanes = lane[:PANEL]
        index = row_of[:PANEL, :1]
        block = aug[pl.ds(first, PANEL), :]
        left = block[:, :rank]
        cols = [
            jnp.sum(jnp.where(lanes == first + k, left, 0.0), axis=1, keepdims=True)
            for k in range(PANEL)
        ]
        scale = jnp.zeros((PANEL, 1), F32)
        for k in range(PANEL):
            inv = 1.0 / cols[k][k : k + 1]
            f = jnp.where(index > k, cols[k] * inv, 0.0)
            for m in range(k + 1, PANEL):
                cols[m] = cols[m] - f * cols[m][k : k + 1]
            block = block - f * block[k : k + 1]
            scale = jnp.where(index == k, inv, scale)
        u = thirds(jnp.where(lanes >= first + PANEL, block[:, :rank] * scale, 0.0))
        v = thirds(block)
        lhs = jnp.concatenate([u[i] for i in (0, 0, 0, 1, 1, 2)], axis=0).astype(BF16)
        rhs = jnp.concatenate([v[i] for i in (0, 1, 2, 0, 1, 0)], axis=0).astype(BF16)
        aug[...] = aug[...] - dot(lhs, rhs, ((0,), (0,)))
        aug[pl.ds(first, PANEL), :] = block
        return 0

    def begin():
        aug[:, :rank] = gram_total()
        aug[:, rank:] = jnp.where(lane == row_of, 1.0, 0.0)

    def chol(first, last):
        lax.fori_loop(first, last, eliminate, 0)

    def finish():
        diag = jnp.sum(jnp.where(lane == row_of, aug[:, :rank], 0.0), axis=1, keepdims=True)
        inverse = aug[:, rank:] * lax.rsqrt(diag)
        inverse_out[...] = inverse
        basis[...] = jnp.sqrt(F32(total_pixels)) * exact(r["sketched"][mine], inverse, ((1,), (1,)))
        projection[...] = exact(r["raw"][...], inverse, ((1,), (1,)))

    def gram_part():
        v = r["sketched"][...]
        return exact(v, v, ((0,), (0,)))

    def raw_part():
        v = r["raw"][...]
        return exact(v, v, ((0,), (0,)))

    gram, gram_total, drain_gram = total_sum(0, gram_part, True)
    spectrum, spectrum_total, drain_spectrum = total_sum(1, raw_part, False)
    panels = rank // PANEL

    def panel(i):
        if i == 0:
            begin()
        chol(panels * i // PARTS, panels * (i + 1) // PARTS)

    def send_own(h):
        in_plane(h, 0)
        if h == 0:
            swap()

    def give_take(h):
        take(h)
        if h == G - 1:
            merge()

    def prepare(s):
        if not prepared:
            swapped()
        prepared.add(s)
        prep(s)

    prepared = set()
    steps = dict(
        ownp=send_own, ownz=to_plane, prep=prepare, zin=zin, ownq=in_plane_rest, zot=in_plane_rest, rst=rs_rest, diag=diag, share=share, fin=multiply, give=give,
        take=give_take, rs1=rs1, rs2=rs2, rs3=rs3, collect=collect, sum=lambda k, i: (gram, spectrum)[k][i](),
        panel=panel, finish=finish,
    )
    for name, *index in schedule(G, Z):
        steps[name](*index)
    spec[...] = spectrum_total()
    finish_sends()


def finish_kernel(patches, basis_in, projection_in, inverse_in, spec_in, basis, projection, spectrum):
    inverse = inverse_in[...]
    basis[...] = basis_in[...]
    projection[...] = projection_in[...]
    spectrum[...] = exact(exact(inverse, spec_in[...]), inverse, ((1,), (1,))) / F32(patches)


def body(grid, green, sketch):
    C, X, Y, Z = grid
    rows, rank = sketch.shape
    pixels, patches = green.shape
    G, deep, half, keep = layout_of(grid, rows, rank)
    other = deep - half
    both = C * pixels
    few = rank // (X * Y)

    def vmem(*shape):
        return pltpu.VMEM(shape, F32)

    def packed(*shape):
        return pltpu.VMEM(shape, BF16)

    def dma(*shape):
        return pltpu.SemaphoreType.DMA(shape)

    flags = pltpu.SemaphoreType.REGULAR((Z,))
    links = X - 1 + Y - 1 + (X - 1) * (Y - 1)
    count = 2 * G * deep * ((Z + 1) * links + Z - 1) + G * both
    scratch = dict(
        green=vmem(both, patches), sketch=vmem(rows, rank), gat=vmem(G, Z, Y, X, deep, rank),
        turned=vmem(X * Y * C * rows, both),
        gl=packed(Z, X * Y, 2 * G * both, deep), gt=packed(Z, X * Y, deep, 2 * G * both),
        acc=vmem(G, G * both, rank), mine=vmem(G, both, rank), theirs=vmem(G, both, rank),
        folded=vmem(G, both, rank), weights=packed(G, 2, 2 * G * both, rank), sketched=vmem(both, rank),
        part=vmem(G, Z, Y, X, deep, rank),
        rda=vmem(G, Z, Y, X, half, rank), rdb=vmem(G, Z, Y, X, other, rank),
        rya=vmem(G, Z, Y, half, rank), rxb=vmem(G, Z, X, other, rank),
        rxa=vmem(G, Z, X, half, rank), ryb=vmem(G, Z, Y, other, rank),
        ebuf=vmem(G, Y, X, max(8, deep - 2 * (keep or 0)), rank),
        fin=vmem(G, Z, deep, rank), rz=vmem(G, Z, deep, rank), raw=vmem(rows, rank),
        t_src=vmem(2, X * Y, few, rank), t_in=vmem(2, C, X * Y, few, rank),
        t_top=vmem(2, Z, few, rank), t_res=vmem(2, X * Y, few, rank),
        aug=vmem(rank, 2 * rank), kup=flags, kdown=flags,
        tally=vmem(count, rank),
        send=dma(1), load=dma(2), swap=dma(1 + G), swap_send=dma(1),
        agz=dma(G, Z), agf=dma(G, Z), agr=dma(G, Z),
        rsf=dma(G, Z), rsr=dma(G, Z), rsz=dma(G), age=dma(G), rse=dma(G), sums=dma(2, 3), sums_send=dma(2),
    )
    total_pixels = pixels * C * X * Y * Z
    tall = jax.ShapeDtypeStruct((pixels, rank), F32)
    wide = jax.ShapeDtypeStruct((rows, rank), F32)
    square = jax.ShapeDtypeStruct((rank, rank), F32)
    whole = pl.BlockSpec(memory_space=pltpu.VMEM)
    parts = pl.pallas_call(
        functools.partial(kernel, grid, total_pixels),
        out_shape=(tall, wide, square, square),
        in_specs=[pl.BlockSpec(memory_space=pl.ANY)] * 2,
        out_specs=(whole,) * 4,
        scratch_shapes=[scratch],
        compiler_params=pltpu.CompilerParams(
            collective_id=0, has_side_effects=True, vmem_limit_bytes=int(VLIM * 2**20)
        ),
    )(green, sketch)
    return pl.pallas_call(
        functools.partial(finish_kernel, patches),
        out_shape=(tall, wide, square),
        in_specs=[whole] * 4,
        out_specs=(whole,) * 3,
        compiler_params=pltpu.CompilerParams(vmem_limit_bytes=2**20),
    )(*parts)


def solution(mesh):
    grid = grid_of(mesh.shape["pix"])
    in_specs = (P("pix", None), P("pix", None))
    out_specs = (P("pix", None), P("pix", None), P())
    return jax.shard_map(
        functools.partial(body, grid), mesh=mesh, in_specs=in_specs, out_specs=out_specs, check_vma=False
    )
```
